256 devices in a mesh: parts: 2 (over y), dp: 64 (over x, z), tensor: 2 (over core).
Axes of the slice: x: 4, y: 2, z: 16, core: 2. Of those that a mesh axis runs over, the one named last changes fastest.
The devices are a block of a 4x16x16 slice.
Arguments:
- normed: bfloat16 [128, 256, 4096], P(('parts', 'dp')), parts along dimension 0, may hold values from -28 to 28
- q_weight: bfloat16 [4096, 2048], P('dp', 'tensor'), may hold values from -0.09375 to 0.09375
- kv_weight: bfloat16 [4096, 2, 512], P('dp', None, 'tensor'), may hold values from -0.09375 to 0.09375
- o_weight: bfloat16 [2048, 4096], P('tensor', 'dp'), may hold values from -0.5 to 0.5
- lengths: int32 [128], P(('parts', 'dp')), parts along dimension 0, may hold values from 64 to 256
- destinations: int32 [128], P(('parts', 'dp')), parts along dimension 0, may hold values from 0 to 63, each once
Outputs:
- projected: bfloat16 [128, 256, 4096], P(('parts', 'dp'), None, 'tensor'), parts along dimension 0
- kv_cache: bfloat16 [128, 2, 4, 256, 128], P(('parts', 'dp'), None, None, 'tensor'), parts along dimension 0
The draws below stay inside these ranges and needn't reach their ends.
There are 2 independent parts, one for each index of `parts`. The reference program is written for one: setup_inputs(seed, part) draws one part's arguments, and reference() takes and returns one part's arrays. A program takes and returns all parts, laid end to end along the dimension named above; an argument that names none is the same for every part. Nothing has to cross between parts.
All inputs are finite; a program needn't handle non-finite values.
Results may differ from the reference program's by a relative error of at most 0.012.
The reference program's roundings to bfloat16 on the way (of `query`, `keys`, `weights`, `attended` and `cache`) count: a program that leaves them out, or rounds other values in their place, can miss the bound.
Values may be sent and summed in bfloat16 or wider, within the bound.
A program may use at most 128 MiB of HBM per device.

```python
import math
import jax
import jax.numpy as jnp
from jax import lax

D = 4096
HD = 128
HEADS = 16
KV_HEADS = 4
LEN = 256
PROMPTS = 64


def draw_normed(key, part):
    shape = (PROMPTS, LEN, D)
    base_key = jax.random.fold_in(key, 11)
    values = jax.random.truncated_normal(base_key, -6.0, 6.0, shape, jnp.float32)
    return values.astype(jnp.bfloat16)


def touch_ends(drawn, stream_key, low, high):
    dims = drawn.shape
    place = [jax.random.randint(jax.random.fold_in(stream_key, axis), (), 0, dims[axis]) for axis in range(len(dims))]
    drawn = drawn.at[tuple(place)].set(low)
    longest = dims.index(max(dims))
    place[longest] = (place[longest] + 1) % dims[longest]
    return drawn.at[tuple(place)].set(high)


def level_of(key, extent, split, smallest, top_value):
    factor_of = 1.0
    for dim, blocks in split:
        draws = jax.random.uniform(jax.random.fold_in(jax.random.fold_in(key, 6), dim), (blocks,), jnp.float32, smallest / len(split), top_value / len(split))
        factor_of = factor_of * jnp.repeat(jnp.exp(draws), extent[dim] // blocks).reshape((-1,) + (1,) * (len(extent) - 1 - dim))
    return factor_of


def scatter_about(stream_key, shape, deviation, bound, shards=(), kind=jnp.bfloat16):
    loudness = level_of(stream_key, shape, shards, -0.22, 0.18) if shards else 1.0
    result = jax.random.normal(stream_key, shape, jnp.float32) * deviation * loudness
    return jnp.minimum(jnp.maximum(result, -bound), bound).astype(kind)


def setup_inputs(seed: int = 0, part: int = 0) -> dict:
    key_list = jax.random.split(jax.random.key(seed), 7)
    part_splits = jax.random.split(jax.random.fold_in(key_list[6], part), 7)
    normed = draw_normed(jax.random.fold_in(jax.random.fold_in(key_list[6], part), 71), part)
    q_weight = scatter_about(key_list[1], (D, HEADS * HD), D ** -0.5, 0.09375, ((0, 64), (1, 2)))
    kv_weight = scatter_about(key_list[2], (D, 2, KV_HEADS * HD), D ** -0.5, 0.09375, ((0, 64), (2, 2)))
    o_weight = scatter_about(key_list[3], (HEADS * HD, D), HD ** -0.5, 0.5, ((0, 2), (1, 64)))
    lengths = touch_ends(jax.random.randint(part_splits[4], (PROMPTS,), LEN // 4, LEN + 1), jax.random.fold_in(part_splits[4], 1), LEN // 4, LEN).astype(jnp.int32)
    destinations = jax.random.permutation(part_splits[5], PROMPTS).astype(jnp.int32)
    return dict(normed=normed, q_weight=q_weight, kv_weight=kv_weight, o_weight=o_weight, lengths=lengths, destinations=destinations)


ROPE_BASE = 500000.0

def rotate(values, positions):
    half = values.shape[-1] // 2
    steps = jnp.arange(half, dtype=jnp.float32) * (2.0 / values.shape[-1])
    freq = jnp.power(jnp.float32(ROPE_BASE), -steps)
    angle = positions.astype(jnp.float32)[:, None] * freq[None, :]
    cosine = jnp.cos(angle)[:, None, :]
    sine = jnp.sin(angle)[:, None, :]
    first = values[..., :half]
    second = values[..., half:]
    return jnp.concatenate([first * cosine - second * sine, second * cosine + first * sine], axis=-1)

def reference(normed, q_weight, kv_weight, o_weight, lengths, destinations):

    def one_prompt(item):
        tokens, length = item
        total = tokens.shape[0]
        positions = jnp.arange(total, dtype=jnp.int32)
        query = jnp.dot(tokens, q_weight, preferred_element_type=jnp.float32).reshape(total, HEADS, HD)
        query = rotate(query, positions).astype(jnp.bfloat16)
        pair = jnp.dot(tokens, kv_weight.reshape(D, 2 * KV_HEADS * HD), preferred_element_type=jnp.float32)
        pair = pair.reshape(total, 2, KV_HEADS, HD)
        keys = rotate(pair[:, 0], positions).astype(jnp.bfloat16)
        values = pair[:, 1].astype(jnp.bfloat16)
        group = HEADS // KV_HEADS
        grouped = query.reshape(total, KV_HEADS, group, HD).transpose(1, 2, 0, 3).astype(jnp.float32)
        key_rows = keys.transpose(1, 0, 2).astype(jnp.float32)
        value_rows = values.transpose(1, 0, 2).astype(jnp.float32)
        scores = jnp.einsum('kgqd,ktd->kgqt', grouped, key_rows, precision=lax.Precision.HIGHEST) / math.sqrt(HD)
        allowed = (positions[:, None] >= positions[None, :]) & (positions[None, :] < length)
        scores = jnp.where(allowed, scores, -jnp.inf)
        peak = lax.optimization_barrier(jnp.max(scores, axis=-1, keepdims=True))
        expo = jnp.exp(scores - peak)
        weights = (expo / lax.optimization_barrier(jnp.sum(expo, axis=-1, keepdims=True))).astype(jnp.bfloat16)
        attended = jnp.einsum('kgqt,ktd->kgqd', weights.astype(jnp.float32), value_rows, precision=lax.Precision.HIGHEST)
        attended = attended.astype(jnp.bfloat16).transpose(2, 0, 1, 3).reshape(total, HEADS * HD)
        projected = jnp.dot(attended, o_weight, preferred_element_type=jnp.float32).astype(jnp.bfloat16)
        live = (positions < length)[:, None, None]
        kept_keys = jnp.where(live, keys, jnp.zeros_like(keys))
        kept_values = jnp.where(live, values, jnp.zeros_like(values))
        cache = jnp.stack([kept_keys, kept_values], axis=0).transpose(0, 2, 1, 3)
        return (projected, cache)
    projected, caches = lax.map(one_prompt, (normed, lengths))
    slots = jnp.arange(PROMPTS, dtype=jnp.int32)
    match = destinations[None, :] == slots[:, None]
    source = lax.optimization_barrier(jnp.sum(jnp.where(match, slots[None, :], 0), axis=1)).astype(jnp.int32)
    return (projected, jnp.take(caches, source, axis=0))
```

```python
import functools
import math

import jax
import jax.numpy as jnp
from jax import lax
from jax.experimental import pallas as pl
from jax.experimental.pallas import tpu as pltpu
from jax.sharding import PartitionSpec as P

HD = 128
ROPE_BASE = 500000.0
NX = 4
KC = 512
QC = 64


def tables(total):
    half = HD // 2
    steps = jnp.arange(half, dtype=jnp.float32) * (2.0 / HD)
    freq = jnp.power(jnp.float32(ROPE_BASE), -steps)
    angle = jnp.arange(total, dtype=jnp.float32)[:, None] * freq[None, :]
    cosine, sine = jnp.cos(angle), jnp.sin(angle)
    return (
        jnp.concatenate([cosine, cosine], axis=-1),
        jnp.concatenate([-sine, sine], axis=-1),
    )


def remote(src, dst, send, recv, device):
    return pltpu.make_async_remote_copy(
        src_ref=src,
        dst_ref=dst,
        send_sem=send,
        recv_sem=recv,
        device_id=device,
        device_id_type=pl.DeviceIdType.MESH,
    )


def kernel(
    nz, x_hbm, wcat, o_t, cos_ref, sin_ref, meta_ref, out_hbm, kv_hbm,
    wbuf, wobuf, xbuf, att, acc, oacc, obuf, meta, dests, srcv, srcs, kvall, swap, spread, perm, heads,
    meta_s, meta_r, w0_s, w0_r, ring_s, ring_r, sib_s, sib_r, y_s, y_r, ysib_s, ysib_r, own_s, own_r,
    o_s, o_r, osib_s, osib_r, oown_s, oown_r, x_l, x_s, xf_s, x_r, a_s, af_s, a_r, swap_s, swap_r,
    dest_s, dest_r, c1_s, c1_r, src_l, c2_s, c2_r, c3_s, c3_r, c3_l, out_s, out_r, out_l,
):
    part, dp, c = lax.axis_index("parts"), lax.axis_index("dp"), lax.axis_index("tensor")
    x, z = lax.div(dp, nz), lax.rem(dp, nz)
    half = nz // 2
    yb = lax.rem(part, 2)
    mate = part + 1 - 2 * yb
    rows = wcat.shape[1]
    total = xbuf.shape[1]
    piece = total // nz
    last = 2 * (half - 1)

    def at_x(offset, core):
        return (part, lax.rem(x + offset + NX, NX) * nz + z, core)

    def at_z(where, core):
        return (part, x * nz + where, core)

    sibling = (part, dp, 1 - c)
    partner = (mate, dp, c)
    up, down = lax.rem(z + 1, nz), lax.rem(z + nz - 1, nz)

    barrier = pltpu.get_barrier_semaphore()
    greeted = [at_x(o, k) for o in range(1, NX) for k in (0, 1)]
    greeted += [sibling, partner, at_z(up, c), at_z(down, c)]
    for device in greeted:
        pl.semaphore_signal(barrier, inc=1, device_id=device, device_id_type=pl.DeviceIdType.MESH)
    pl.semaphore_wait(barrier, len(greeted))

    def w_block(xs, zs):
        return wbuf.at[pl.ds(pl.multiple_of((xs * nz + zs) * rows, rows), rows), :]

    def w0(b):
        return remote(
            wcat.at[b], w_block(x, z), w0_s.at[b], w0_r.at[lax.rem(x, 2)],
            (part, (2 * c + b) * nz + z, lax.div(x, 2)),
        )

    def w0_here(b):
        return pltpu.make_async_copy(wcat.at[b], w_block(x, z), w0_s.at[b])

    for b in (0, 1):
        pl.when(2 * c + b != x)(lambda b=b: w0(b).start())

    for b in (0, 1):
        @pl.when(2 * c + b == x)
        def _(b=b):
            w_block(x, z)[...] = wcat[b]

    meta[x] = meta_ref[...]

    def meta_copy(o):
        return remote(meta_ref, meta.at[x], meta_s.at[o], meta_r.at[o], at_x(o, c))

    for o in range(1, NX):
        meta_copy(o).start()

    quarter = total // 4
    away = [lax.rem(x - 2 * c - s + 2 * NX, NX) for s in (0, 1)]
    is_source = lax.div(x, 2) == c
    mine = lax.rem(x, 2)

    def x_rows(q):
        return pl.ds(q * quarter, quarter)

    def x_send(direction, q):
        return remote(
            x_hbm.at[x_rows(q)], xbuf.at[mine, x_rows(q)], x_s.at[direction, q], x_r.at[mine, q],
            at_x(1 if direction == 0 else -1, c),
        )

    def x_local():
        return pltpu.make_async_copy(x_hbm, xbuf.at[mine], x_l)

    def x_forward(s, q, direction):
        return remote(
            xbuf.at[s, x_rows(q)], xbuf.at[s, x_rows(q)], xf_s.at[s, q % 2], x_r.at[s, q],
            at_x(1 if direction == 0 else -1, c),
        )

    @pl.when(is_source)
    def _():
        for i in range(4):
            x_send(0, i).start()
            x_send(1, (i + 2) % 4).start()
        x_local().start()

    def pass_on(i):
        for s in (0, 1):
            @pl.when(away[s] == 1)
            def _(s=s):
                x_forward(s, i, 0).wait_recv()
                x_forward(s, i, 0).start()

            @pl.when(away[s] == 3)
            def _(s=s):
                x_forward(s, 2 + i, 1).wait_recv()
                x_forward(s, 2 + i, 1).start()

    def hop(direction, zs, idx):
        blk = w_block(2 * c + yb, zs)
        return remote(blk, blk, ring_s.at[idx], ring_r.at[idx], at_z(up if direction == 0 else down, c))

    def to_sibling(zs, idx):
        blk = w_block(2 * c + yb, zs)
        return remote(blk, blk, sib_s.at[idx], sib_r.at[idx], sibling)

    def from_sibling(zs, idx):
        blk = w_block(2 * (1 - c) + yb, zs)
        return remote(blk, blk, sib_s.at[idx], sib_r.at[idx], sibling)

    def to_partner(zs, idx):
        blk = w_block(2 * c + yb, zs)
        return remote(blk, blk, y_s.at[idx], y_r.at[idx], partner)

    def from_partner(zs, idx):
        blk = w_block(2 * c + 1 - yb, zs)
        return remote(blk, blk, y_s.at[idx], y_r.at[idx], partner)

    def y_to_sibling(zs, idx):
        blk = w_block(2 * c + 1 - yb, zs)
        return remote(blk, blk, ysib_s.at[idx], ysib_r.at[idx], sibling)

    def own_to_sibling(i):
        blk = w_block(2 * c + i, z)
        return remote(blk, blk, own_s.at[i], own_r.at[i], sibling)

    def o_block(zs, core):
        return wobuf.at[core, pl.ds(pl.multiple_of(zs * QC, QC), QC), :]

    def o_hop(direction, zs, idx, src=None):
        blk = o_block(zs, c)
        return remote(
            blk if src is None else src, blk, o_s.at[idx], o_r.at[idx],
            at_z(up if direction == 0 else down, c),
        )

    def o_sibling(zs, idx):
        blk = o_block(zs, c)
        return remote(blk, blk, osib_s.at[idx], osib_r.at[idx], sibling)

    def o_own_sibling():
        return remote(o_t, o_block(z, c), oown_s, oown_r, sibling)

    for i in (0, 1):
        @pl.when(2 * c + i != x)
        def _(i=i):
            remote(wcat.at[0], w_block(2 * c + i, z), w0_s.at[0], w0_r.at[i], sibling).wait_recv()

    first = (0, half - 1)
    for direction in (0, 1):
        hop(direction, z, first[direction]).start()
    for i in (0, 1):
        own_to_sibling(i).start()
    for direction in (0, 1):
        o_hop(direction, z, first[direction], o_t).start()
    o_own_sibling().start()
    o_block(z, c)[...] = o_t[...]

    def block_of(direction, k):
        return lax.rem(z + (nz - k if direction == 0 else k), nz)

    def partner_on(direction, k, idx):
        zs = block_of(direction, k)
        from_partner(zs, idx).wait_recv()
        y_to_sibling(zs, idx).start()

    def ring_step(k, carry):
        for direction in (0, 1):
            idx = direction * (half - 1) + k - 1
            nxt = jnp.where(k == half - 1, last, idx + 1)
            zs = block_of(direction, k)
            hop(direction, zs, idx).wait_recv()

            @pl.when((k < half - 1) | (c == direction))
            def _():
                hop(direction, zs, nxt).start()

            to_sibling(zs, idx).start()
            to_partner(zs, idx).start()
        for direction in (0, 1):
            idx = direction * (half - 1) + k - 1
            nxt = jnp.where(k == half - 1, last, idx + 1)
            zs = block_of(direction, k)
            o_hop(direction, zs, idx).wait_recv()

            @pl.when((k < half - 1) | (c == direction))
            def _():
                o_hop(direction, zs, nxt).start()

            o_sibling(zs, idx).start()

        @pl.when(k > 1)
        def _():
            for direction in (0, 1):
                partner_on(direction, k - 1, direction * (half - 1) + k - 2)

        return carry

    lax.fori_loop(1, 3, ring_step, 0)
    pass_on(0)
    lax.fori_loop(3, 5, ring_step, 0)
    pass_on(1)
    lax.fori_loop(5, half, ring_step, 0)
    far = block_of(0, half)
    hop(0, far, last).wait_recv()
    to_sibling(far, last).start()
    to_partner(far, last).start()
    for direction in (0, 1):
        partner_on(direction, half - 1, direction * (half - 1) + half - 2)
    o_hop(0, far, last).wait_recv()
    o_sibling(far, last).start()
    from_partner(far, last).wait_recv()
    y_to_sibling(far, last).start()

    def arrived(idx, carry):
        from_sibling(z, idx).wait_recv()
        remote(w_block(2 * c, z), w_block(2 * c, z), ysib_s.at[idx], ysib_r.at[idx], sibling).wait_recv()
        remote(o_block(z, c), o_block(z, c), osib_s.at[idx], osib_r.at[idx], sibling).wait_recv()
        return carry

    lax.fori_loop(0, last + 1, arrived, 0)
    for i in (0, 1):
        own_to_sibling(i).wait_recv()
    o_own_sibling().wait_recv()
    for s in (0, 1):
        @pl.when(away[s] == 1)
        def _(s=s):
            for q in (2, 3):
                x_forward(s, q, 0).wait_recv()

        @pl.when(away[s] == 3)
        def _(s=s):
            for q in (0, 1):
                x_forward(s, q, 0).wait_recv()

        @pl.when(away[s] == 2)
        def _(s=s):
            for q in range(4):
                x_forward(s, q, 0).wait_recv()

    @pl.when(is_source)
    def _():
        x_local().wait()

    for o in range(1, NX):
        meta_copy(o).wait_recv()

    lane = lax.broadcasted_iota(jnp.int32, (1, HD), 1)
    row = jnp.zeros((1, HD), jnp.int32)
    for j in range(NX):
        row = jnp.where(lane == j, meta[j, pl.ds(0, 1), :], row)
    dests[z] = row

    cosine, sine = cos_ref[...], sin_ref[...]

    def rotated(u):
        return u * cosine + pltpu.roll(u, HD // 2, 1) * sine

    groups = (acc.shape[1] - 2 * HD) // HD
    key_at = lax.broadcasted_iota(jnp.int32, (total, total), 1)
    query_at = lax.broadcasted_iota(jnp.int32, (total, total), 0)
    position = lax.broadcasted_iota(jnp.int32, (total, HD), 0)

    def a_send(s, direction):
        return remote(
            att.at[s, x], att.at[s, x], a_s.at[s, direction], a_r.at[s, direction],
            at_x(1 if direction == 0 else -1, c),
        )

    def a_forward(s):
        blk = att.at[s, lax.rem(x + (NX - 1 if s == 0 else 1), NX)]
        return remote(blk, blk, af_s.at[s], a_r.at[s, 2], at_x(1 if s == 0 else -1, c))

    for s in (0, 1):
        acc[...] = jnp.zeros_like(acc)

        def project(i, carry, s=s):
            cols = pl.ds(pl.multiple_of(i * KC, KC), KC)
            acc[...] += jnp.dot(xbuf[s, :, cols], wbuf[cols, :], preferred_element_type=jnp.float32)
            return carry

        lax.fori_loop(0, wbuf.shape[0] // KC, project, 0)
        length = meta[2 * c + s, pl.ds(1, 1), :]
        keys = rotated(acc[:, groups * HD : (groups + 1) * HD])
        values = acc[:, (groups + 1) * HD :]
        live = position < length
        kept_keys = jnp.where(live, keys, 0.0).astype(jnp.bfloat16)
        kept_values = jnp.where(live, values, 0.0).astype(jnp.bfloat16)

        @pl.when(c == 0)
        def _(s=s, kept_keys=kept_keys, kept_values=kept_values):
            kvall[s] = kept_keys
            swap[s] = kept_values

        @pl.when(c == 1)
        def _(s=s, kept_keys=kept_keys, kept_values=kept_values):
            kvall[2 + s] = kept_values
            swap[s] = kept_keys

        keys = keys.astype(jnp.bfloat16)
        values = values.astype(jnp.bfloat16)
        wide = jnp.concatenate([length] * (total // HD), axis=1)
        allowed = (query_at >= key_at) & (key_at < wide)
        for g in range(groups):
            query = rotated(acc[:, g * HD : (g + 1) * HD]).astype(jnp.bfloat16)
            scores = lax.dot_general(
                query, keys, (((1,), (1,)), ((), ())), preferred_element_type=jnp.float32
            ) * (1.0 / math.sqrt(HD))
            scores = jnp.where(allowed, scores, -jnp.inf)
            expo = jnp.exp(scores - jnp.max(scores, axis=1, keepdims=True))
            weights = (expo / jnp.sum(expo, axis=1, keepdims=True)).astype(jnp.bfloat16)
            att[s, x, :, g * HD : (g + 1) * HD] = jnp.dot(
                weights, values, preferred_element_type=jnp.float32
            ).astype(jnp.bfloat16)
        for direction in (0, 1):
            a_send(s, direction).start()

    def swapped():
        return remote(swap, kvall.at[pl.ds(2 * c, 2)], swap_s, swap_r, sibling)

    swapped().start()

    def d_copy(o):
        return remote(dests.at[z], dests.at[z], dest_s.at[o], dest_r.at[o], at_z(lax.rem(z + o, nz), c))

    def c1_copy(o):
        to = lax.rem(z + o, nz)
        return remote(
            kvall.at[:, pl.ds(pl.multiple_of(to * piece, piece), piece), :],
            spread.at[pl.ds(z * NX, NX)],
            c1_s.at[o], c1_r.at[o], at_z(to, c),
        )

    def send_dest(o, carry):
        d_copy(o).start()
        return carry

    lax.fori_loop(1, nz, send_dest, 0)
    swapped().wait_recv()

    def send_c1(o, carry):
        c1_copy(o).start()
        return carry

    lax.fori_loop(1, nz, send_c1, 0)
    spread[pl.ds(z * NX, NX)] = kvall[:, pl.ds(pl.multiple_of(z * piece, piece), piece), :]

    def head_rows(s, xs):
        core = lax.div(xs, 2)
        cols = pl.ds(pl.multiple_of(lax.rem(xs, 2) * att.shape[3], att.shape[3]), att.shape[3])
        return lax.dot_general(
            att[s, xs], wobuf[core, :, cols], (((1,), (1,)), ((), ())),
            preferred_element_type=jnp.float32,
        )

    for s in (0, 1):
        oacc[s] = head_rows(s, x)
    for s in (0, 1):
        for direction in (0, 1):
            a_send(s, direction).wait_recv()
            if direction == s:
                a_forward(s).start()
    for s in (0, 1):
        for direction in (0, 1):
            oacc[s] += head_rows(s, lax.rem(x + (NX - 1 if direction == 0 else 1), NX))

    def d_wait(o, carry):
        d_copy(o).wait_recv()
        c1_copy(o).wait_recv()
        return carry

    lax.fori_loop(1, nz, d_wait, 0)
    all_dests = dests[...].reshape(nz, HD)
    lanes = lax.broadcasted_iota(jnp.int32, (nz, HD), 1)
    prompt = lax.broadcasted_iota(jnp.int32, (nz, HD), 0) * NX
    source = jnp.zeros((nz, HD), jnp.int32)
    for j in range(NX):
        slot = jnp.sum(jnp.where(lanes == j, all_dests, 0), axis=1, keepdims=True)
        source += jnp.where(slot == lanes, prompt + j, 0)
    srcv[...] = jnp.minimum(jnp.sum(source, axis=0, keepdims=True), NX * nz - 1)
    to_scalars = pltpu.make_async_copy(srcv, srcs, src_l)
    to_scalars.start()
    to_scalars.wait()

    def reorder(d, carry):
        perm[d] = spread[srcs[0, d]]
        return carry

    lax.fori_loop(0, NX * nz, reorder, 0)

    def c2_copy(o):
        to = lax.rem(x + o, NX)
        return remote(
            perm.at[pl.ds(to * nz, nz)], heads.at[x], c2_s.at[o], c2_r.at[o], at_x(o, c)
        )

    for o in range(1, NX):
        c2_copy(o).start()
    heads[x] = perm[pl.ds(x * nz, nz)]

    width = oacc.shape[2]

    def out_copy(s):
        to = 2 * c + s
        cols = pl.ds(pl.multiple_of(lax.rem(x, 2) * width, width), width)
        return remote(
            obuf.at[s], out_hbm.at[:, cols], out_s.at[s], out_r.at[lax.rem(x, 2)],
            (part, to * nz + z, lax.div(x, 2)),
        )

    def out_here(s):
        cols = pl.ds(pl.multiple_of(lax.rem(x, 2) * width, width), width)
        return pltpu.make_async_copy(obuf.at[s], out_hbm.at[:, cols], out_l)

    for s in (0, 1):
        a_forward(s).wait_recv()
        obuf[s] = (oacc[s] + head_rows(s, lax.rem(x + 2, NX))).astype(jnp.bfloat16)
        pl.when(2 * c + s != x)(lambda s=s: out_copy(s).start())
        pl.when(2 * c + s == x)(lambda s=s: out_here(s).start())

    for o in range(1, NX):
        c2_copy(o).wait_recv()
    target = lax.div(z, half)
    place = pl.ds(pl.multiple_of(lax.rem(z, half) * piece, piece), piece)

    def c3_copy(o):
        to = lax.rem(z + o, nz)
        return remote(
            heads.at[:, to], kv_hbm.at[c, :, place, :], c3_s.at[o], c3_r.at[c, lax.rem(z, half)],
            at_z(to, target),
        )

    def c3_here():
        return pltpu.make_async_copy(heads.at[:, z], kv_hbm.at[c, :, place, :], c3_l)

    def send_c3(o, carry):
        c3_copy(o).start()
        return carry

    lax.fori_loop(1, nz, send_c3, 0)
    pl.when(target == c)(lambda: c3_here().start())
    pl.when(target != c)(lambda: c3_copy(0).start())

    def c3_wait(i, carry):
        kind, zs = lax.div(i, half), lax.rem(i, half)

        @pl.when((kind != c) | (half * c + zs != z))
        def _():
            remote(
                heads.at[:, z],
                kv_hbm.at[kind, :, pl.ds(pl.multiple_of(zs * piece, piece), piece), :],
                c3_s.at[0], c3_r.at[kind, zs], sibling,
            ).wait_recv()

        return carry

    lax.fori_loop(0, nz, c3_wait, 0)
    pl.when(target == c)(lambda: c3_here().wait())
    pl.when(target != c)(lambda: c3_copy(0).wait_send())
    for i in (0, 1):
        @pl.when(2 * c + i != x)
        def _(i=i):
            cols = pl.ds(i * width, width)
            remote(obuf.at[0], out_hbm.at[:, cols], out_s.at[0], out_r.at[i], sibling).wait_recv()

    for s in (0, 1):
        pl.when(2 * c + s != x)(lambda s=s: out_copy(s).wait_send())
        pl.when(2 * c + s == x)(lambda s=s: out_here(s).wait())
        for direction in (0, 1):
            a_send(s, direction).wait_send()
        a_forward(s).wait_send()
    for b in (0, 1):
        pl.when(2 * c + b != x)(lambda b=b: w0(b).wait_send())
    for o in range(1, NX):
        meta_copy(o).wait_send()
        c2_copy(o).wait_send()

    @pl.when(is_source)
    def _():
        for i in range(4):
            for direction in (0, 1):
                x_send(direction, i).wait_send()

    for s in (0, 1):
        for i in (0, 1):
            pl.when(away[s] == 1)(lambda s=s, i=i: x_forward(s, i, 0).wait_send())
            pl.when(away[s] == 3)(lambda s=s, i=i: x_forward(s, 2 + i, 1).wait_send())
        own_to_sibling(s).wait_send()
    o_own_sibling().wait_send()
    swapped().wait_send()

    def drain_z(o, carry):
        d_copy(o).wait_send()
        c1_copy(o).wait_send()
        c3_copy(o).wait_send()
        return carry

    lax.fori_loop(1, nz, drain_z, 0)

    def drain_ring(idx, carry):
        hop(0, z, idx).wait_send()
        to_sibling(z, idx).wait_send()
        to_partner(z, idx).wait_send()
        y_to_sibling(z, idx).wait_send()
        o_hop(0, z, idx).wait_send()
        o_sibling(z, idx).wait_send()
        return carry

    lax.fori_loop(0, last + 1, drain_ring, 0)


def on_device(normed, q_weight, kv_weight, o_weight, lengths, destinations):
    tokens = normed[0]
    total, width = tokens.shape
    nz = lax.axis_size("dp") // NX
    rows = q_weight.shape[0]
    q_cols = q_weight.shape[1] // 2
    q_parts = q_weight.reshape(rows, 2, q_cols).transpose(1, 0, 2)
    kv_parts = kv_weight.reshape(rows, 2, 2, HD).transpose(2, 0, 1, 3).reshape(2, rows, 2 * HD)
    wcat = jnp.concatenate([q_parts, kv_parts], axis=-1)
    o_t = o_weight.T
    cosine, sine = tables(total)
    meta = jnp.stack(
        [jnp.broadcast_to(destinations, (HD,)), jnp.broadcast_to(lengths, (HD,))]
    )
    columns = q_cols + 2 * HD
    o_cols = rows * nz
    piece = total // nz
    hops = nz - 1
    bf16, f32 = jnp.bfloat16, jnp.float32
    dma = pltpu.SemaphoreType.DMA
    scratch = [
        pltpu.VMEM((width, columns), bf16),
        pltpu.VMEM((2, o_cols, o_weight.shape[0]), bf16),
        pltpu.VMEM((2, total, width), bf16),
        pltpu.VMEM((2, NX, total, q_cols), bf16),
        pltpu.VMEM((total, columns), f32),
        pltpu.VMEM((2, total, o_cols), f32),
        pltpu.VMEM((2, total, o_cols), bf16),
        pltpu.VMEM((NX, 2, HD), jnp.int32),
        pltpu.VMEM((nz, 1, HD), jnp.int32),
        pltpu.VMEM((1, HD), jnp.int32),
        pltpu.SMEM((1, HD), jnp.int32),
        pltpu.VMEM((NX, total, HD), bf16),
        pltpu.VMEM((2, total, HD), bf16),
        pltpu.VMEM((NX * nz, piece, HD), bf16),
        pltpu.VMEM((NX * nz, piece, HD), bf16),
        pltpu.VMEM((NX, nz, piece, HD), bf16),
    ]
    shapes = [
        (NX,), (NX,), (2,), (2,), (hops,), (hops,), (hops,), (hops,), (hops,), (hops,), (hops,), (hops,), (2,), (2,),
        (hops,), (hops,), (hops,), (hops,), None, None, None, (2, 4), (2, 2), (2, 4), (2, 2), (2,), (2, 3), None, None,
        (nz,), (nz,), (nz,), (nz,), None, (NX,), (NX,), (nz,), (2, nz // 2), None, (2,), (2,), None,
    ]
    scratch += [dma if shape is None else dma(shape) for shape in shapes]
    vmem = pl.BlockSpec(memory_space=pltpu.VMEM)
    any_space = pl.BlockSpec(memory_space=pl.ANY)
    projected, cache = pl.pallas_call(
        functools.partial(kernel, nz),
        out_shape=(
            jax.ShapeDtypeStruct((total, 2 * o_cols), bf16),
            jax.ShapeDtypeStruct((2, NX, total // 2, HD), bf16),
        ),
        in_specs=[any_space, vmem, vmem, vmem, vmem, vmem],
        out_specs=(any_space, any_space),
        scratch_shapes=scratch,
        compiler_params=pltpu.CompilerParams(
            collective_id=0, has_side_effects=True, vmem_limit_bytes=60 * 1024 * 1024
        ),
    )(tokens, wcat, o_t, cosine, sine, meta)
    return (projected[None], cache[None])


def solution(mesh):
    placed = (
        P(("parts", "dp"), None, None),
        P("dp", "tensor"),
        P("dp", None, "tensor"),
        P("tensor", "dp"),
        P(("parts", "dp")),
        P(("parts", "dp")),
    )
    return jax.shard_map(
        on_device,
        mesh=mesh,
        in_specs=placed,
        out_specs=(
            P(("parts", "dp"), None, "tensor"),
            P(("parts", "dp"), None, None, "tensor", None),
        ),
        check_vma=False,
    )
```

```python
import functools
import math

import jax
import jax.numpy as jnp
import numpy as np
from jax import lax
from jax.experimental import pallas as pl
from jax.experimental.pallas import tpu as pltpu
from jax.sharding import PartitionSpec as P

HD = 128
ROPE_BASE = 500000.0
NX = 4
KC = 512
QC = 64
LAG = 1


def tables(total):
    half = HD // 2
    steps = np.arange(half, dtype=np.float32) * np.float32(2.0 / HD)
    freq = np.power(np.float32(ROPE_BASE), -steps)
    angle = np.arange(total, dtype=np.float32)[:, None] * freq[None, :]
    cosine, sine = np.cos(angle), np.sin(angle)
    return (
        jnp.asarray(np.concatenate([cosine, cosine], axis=-1)),
        jnp.asarray(np.concatenate([-sine, sine], axis=-1)),
    )


def remote(src, dst, send, recv, device):
    return pltpu.make_async_remote_copy(
        src_ref=src,
        dst_ref=dst,
        send_sem=send,
        recv_sem=recv,
        device_id=device,
        device_id_type=pl.DeviceIdType.MESH,
    )


def kernel(
    nz, x_hbm, q_ref, kv_ref, o_t, cos_ref, sin_ref, dest_ref, length_ref, out_hbm, kv_hbm,
    wbuf, wobuf, xbuf, att, acc, oacc, obuf, meta, dests, srcv, srcs, kvall, swap, spread, perm, heads,
    meta_s, meta_r, w0_s, w0_r, ring_s, ring_r, sib_s, sib_r, y_s, y_r, ysib_s, ysib_r, own_s, own_r,
    o_s, o_r, osib_s, osib_r, oown_s, oown_r, x_l, x_s, xf_s, x_r, a_s, af_s, a_r, swap_s, swap_r,
    dest_s, dest_r, c1_s, c1_r, src_l, c2_s, c2_r, c3_s, c3_r, c3_l, out_s, out_r, out_l, ready, kvbuf, relay, relay_s, relay_r,
    oy_s, oy_r, oysib_s, oysib_r,
):
    part, dp, c = lax.axis_index("parts"), lax.axis_index("dp"), lax.axis_index("tensor")
    x, z = lax.div(dp, nz), lax.rem(dp, nz)
    half = nz // 2
    yb = lax.rem(part, 2)
    mate = part + 1 - 2 * yb
    rows = q_ref.shape[0]
    total = xbuf.shape[1]
    piece = total // nz
    last = 2 * (half - 1)

    def at_x(offset, core):
        return (part, lax.rem(x + offset + NX, NX) * nz + z, core)

    def at_z(where, core):
        return (part, x * nz + where, core)

    sibling = (part, dp, 1 - c)
    partner = (mate, dp, c)
    up, down = lax.rem(z + 1, nz), lax.rem(z + nz - 1, nz)

    barrier = pltpu.get_barrier_semaphore()

    def greet(semaphore, device):
        pl.semaphore_signal(semaphore, inc=1, device_id=device, device_id_type=pl.DeviceIdType.MESH)

    greeted = [at_x(o, k) for o in range(1, NX) for k in (0, 1)] + [sibling, partner]
    for device in greeted:
        greet(barrier, device)
    pl.when(z != 0)(lambda: greet(barrier, at_z(up, c)))
    pl.when(z == 1)(lambda: greet(barrier, at_z(down, c)))
    pl.semaphore_wait(
        barrier, len(greeted) + jnp.where(z == 1, 0, 1) + jnp.where(z == 0, 1, 0)
    )
    pl.when(z != 1)(lambda: greet(ready.at[0], at_z(down, c)))
    pl.when(z == 0)(lambda: greet(ready.at[1], at_z(up, c)))

    columns = wbuf.shape[1]
    q_cols = columns - 2 * HD

    def w_block(xs, zs):
        return wbuf.at[pl.ds(pl.multiple_of((xs * nz + zs) * rows, rows), rows), :]

    def w0_parts(b):
        return (
            (q_ref, b * q_cols, 0, q_cols),
            (kv_ref, b * HD, q_cols, HD),
            (kv_ref, (2 + b) * HD, q_cols + HD, HD),
        )

    def w0(b):
        block = w_block(x, z)
        return [
            remote(
                src.at[:, pl.ds(start, size)], block.at[:, pl.ds(to, size)], w0_s.at[b, i],
                w0_r.at[lax.rem(x, 2)], (part, (2 * c + b) * nz + z, lax.div(x, 2)),
            )
            for i, (src, start, to, size) in enumerate(w0_parts(b))
        ]

    for b in (0, 1):
        @pl.when(2 * c + b != x)
        def _(b=b):
            for copy in w0(b):
                copy.start()

    for b in (0, 1):
        @pl.when(2 * c + b == x)
        def _(b=b):
            block = w_block(x, z)
            for src, start, to, size in w0_parts(b):
                block[:, to : to + size] = src[:, start : start + size]

    meta[x] = jnp.concatenate(
        [jnp.full((1, HD), dest_ref[0], jnp.int32), jnp.full((1, HD), length_ref[0], jnp.int32)]
    )

    def meta_copy(o):
        return remote(meta.at[x], meta.at[x], meta_s.at[o], meta_r.at[o], at_x(o, c))

    for o in range(1, NX):
        meta_copy(o).start()

    quarter = total // 4

    def away(s):
        return lax.rem(x - 2 * c - s + 2 * NX, NX)

    is_source = lax.div(x, 2) == c
    mine = lax.rem(x, 2)

    def x_rows(q):
        return pl.ds(q * quarter, quarter)

    def x_send(direction, q):
        return remote(
            x_hbm.at[x_rows(q)], xbuf.at[mine, x_rows(q)], x_s.at[direction, q], x_r.at[mine, q],
            at_x(1 if direction == 0 else -1, c),
        )

    def x_local():
        return pltpu.make_async_copy(x_hbm, xbuf.at[mine], x_l)

    def x_forward(s, q, direction):
        return remote(
            xbuf.at[s, x_rows(q)], xbuf.at[s, x_rows(q)], xf_s.at[s, q % 2], x_r.at[s, q],
            at_x(1 if direction == 0 else -1, c),
        )

    @pl.when(is_source)
    def _():
        for i in range(4):
            x_send(0, i).start()
            x_send(1, (i + 2) % 4).start()
        x_local().start()

    def x_arrival(s, q):
        rows_of = xbuf.at[s, x_rows(q)]
        return remote(rows_of, rows_of, xf_s.at[s, q % 2], x_r.at[s, q], sibling)

    def pass_on(i):
        for s in (0, 1):
            @pl.when(away(s) == 1)
            def _(s=s):
                x_forward(s, i, 0).wait_recv()
                x_forward(s, i, 0).start()

            @pl.when(away(s) == 3)
            def _(s=s):
                x_forward(s, 2 + i, 1).wait_recv()
                x_forward(s, 2 + i, 1).start()

    def hop(direction, zs, idx, part_of):
        first_row = ((2 * c + yb) * nz + zs) * rows + part_of * (rows // 2)
        blk = wbuf.at[pl.ds(pl.multiple_of(first_row, rows // 2), rows // 2), :]
        return remote(
            blk, blk, ring_s.at[idx, part_of], ring_r.at[idx, part_of],
            at_z(up if direction == 0 else down, c),
        )

    def to_sibling(zs, idx):
        blk = w_block(2 * c + yb, zs)
        return remote(blk, blk, sib_s.at[idx], sib_r.at[idx], sibling)

    def from_sibling(zs, idx):
        blk = w_block(2 * (1 - c) + yb, zs)
        return remote(blk, blk, sib_s.at[idx], sib_r.at[idx], sibling)

    def to_partner(zs, idx):
        blk = w_block(2 * c + yb, zs)
        return remote(blk, blk, y_s.at[idx], y_r.at[idx], partner)

    def from_partner(zs, idx):
        blk = w_block(2 * c + 1 - yb, zs)
        return remote(blk, blk, y_s.at[idx], y_r.at[idx], partner)

    def y_to_sibling(zs, idx):
        blk = w_block(2 * c + 1 - yb, zs)
        return remote(blk, blk, ysib_s.at[idx], ysib_r.at[idx], sibling)

    def own_to_sibling(i):
        blk = w_block(2 * c + i, z)
        return remote(blk, blk, own_s.at[i], own_r.at[i], sibling)

    def o_block(zs, core):
        return wobuf.at[core, pl.ds(pl.multiple_of(zs * QC, QC), QC), :]

    def o_part(zs, which):
        start = pl.multiple_of(zs * QC + which * (QC // 2), QC // 2)
        return wobuf.at[c, pl.ds(start, QC // 2), :]

    def o_hop(direction, zs, idx, src=None):
        blk = o_part(zs, yb)
        return remote(
            blk if src is None else src, blk, o_s.at[idx], o_r.at[idx],
            at_z(up if direction == 0 else down, c),
        )

    def o_sibling(zs, idx):
        blk = o_part(zs, yb)
        return remote(blk, blk, osib_s.at[idx], osib_r.at[idx], sibling)

    def o_partner(zs, idx):
        blk = o_part(zs, yb)
        return remote(blk, blk, oy_s.at[idx], oy_r.at[idx], partner)

    def o_y_sibling(zs, idx):
        blk = o_part(zs, 1 - yb)
        return remote(blk, blk, oysib_s.at[idx], oysib_r.at[idx], sibling)

    def o_own_sibling():
        return remote(o_t, o_block(z, c), oown_s, oown_r, sibling)

    for i in (0, 1):
        @pl.when(2 * c + i != x)
        def _(i=i):
            blk = w_block(2 * c + i, z)
            remote(blk, blk, w0_s.at[0, 0], w0_r.at[i], sibling).wait_recv()

    first = (0, half - 1)
    for i in (0, 1):
        own_to_sibling(i).start()
    pl.when(z != 0)(lambda: pl.semaphore_wait(ready.at[0], 1))
    for h in (0, 1):
        hop(0, z, first[0], h).start()
    pl.when(z == 1)(lambda: pl.semaphore_wait(ready.at[1], 1))
    for h in (0, 1):
        hop(1, z, first[1], h).start()
    o_block(z, c)[...] = o_t[...]

    def block_of(direction, k):
        return lax.rem(z + (nz - k if direction == 0 else k), nz)

    def slot_of(direction, k):
        return direction * (half - 1) + k - 1

    def partner_on(direction, k, idx):
        zs = block_of(direction, k)
        from_partner(zs, idx).wait_recv()
        y_to_sibling(zs, idx).start()

    def w_half(direction, k, h):
        idx = slot_of(direction, k)
        zs = block_of(direction, k)
        hop(direction, zs, idx, h).wait_recv()

        @pl.when((k < half - 1) | (c == direction))
        def _():
            hop(direction, zs, jnp.where(k == half - 1, last, idx + 1), h).start()

    def w_rest(direction, k):
        idx = slot_of(direction, k)
        zs = block_of(direction, k)
        to_sibling(zs, idx).start()
        to_partner(zs, idx).start()

    def o_step(k):
        for direction in (0, 1):
            idx = slot_of(direction, k)
            zs = block_of(direction, k)
            o_hop(direction, zs, idx).wait_recv()

            @pl.when((k < half - 1) | (c == direction))
            def _(direction=direction, idx=idx, zs=zs):
                o_hop(direction, zs, jnp.where(k == half - 1, last, idx + 1)).start()

            o_sibling(zs, idx).start()

    def ring_step(k, carry):
        for h in (0, 1):
            for direction in (0, 1):
                w_half(direction, k, h)
        for direction in (0, 1):
            w_rest(direction, k)
        @pl.when(k > LAG)
        def _():
            o_step(k - LAG)

        @pl.when(k > 1)
        def _():
            for direction in (0, 1):
                partner_on(direction, k - 1, slot_of(direction, k - 1))

        return carry

    for direction in (0, 1):
        o_hop(direction, z, first[direction], o_t.at[pl.ds(pl.multiple_of(yb * (QC // 2), QC // 2), QC // 2)]).start()
    o_own_sibling().start()
    lax.fori_loop(1, 3, ring_step, 0)
    pass_on(0)
    lax.fori_loop(3, 5, ring_step, 0)
    pass_on(1)
    lax.fori_loop(5, half, ring_step, 0)
    far = block_of(0, half)
    for h in (0, 1):
        hop(0, far, last, h).wait_recv()
    to_sibling(far, last).start()
    to_partner(far, last).start()
    for direction in (0, 1):
        partner_on(direction, half - 1, slot_of(direction, half - 1))
    for k in range(half - LAG, half):
        o_step(k)
    for direction in (0, 1):
        def o_over(k, carry, direction=direction):
            o_partner(block_of(direction, k), slot_of(direction, k)).start()
            return carry

        lax.fori_loop(1, half, o_over, 0)
    from_partner(far, last).wait_recv()
    y_to_sibling(far, last).start()

    def arrived(idx, carry):
        from_sibling(z, idx).wait_recv()
        remote(w_block(2 * c, z), w_block(2 * c, z), ysib_s.at[idx], ysib_r.at[idx], sibling).wait_recv()
        return carry

    lax.fori_loop(0, last + 1, arrived, 0)
    for i in (0, 1):
        own_to_sibling(i).wait_recv()
    for o in range(1, NX):
        meta_copy(o).wait_recv()

    lane = lax.broadcasted_iota(jnp.int32, (1, HD), 1)
    row = jnp.zeros((1, HD), jnp.int32)
    for j in range(NX):
        row = jnp.where(lane == j, meta[j, pl.ds(0, 1), :], row)
    dests[z] = row

    cosine, sine = cos_ref[...], sin_ref[...]

    def rotated(u):
        return u * cosine + pltpu.roll(u, HD // 2, 1) * sine

    groups = q_cols // HD
    key_at = lax.broadcasted_iota(jnp.int32, (total, total), 1)
    query_at = lax.broadcasted_iota(jnp.int32, (total, total), 0)
    position = lax.broadcasted_iota(jnp.int32, (total, HD), 0)

    def a_send(s, direction):
        return remote(
            att.at[s, x], att.at[s, x], a_s.at[s, direction], a_r.at[s, direction],
            at_x(1 if direction == 0 else -1, c),
        )

    def a_forward(s):
        blk = att.at[s, lax.rem(x + (NX - 1 if s == 0 else 1), NX)]
        return remote(blk, blk, af_s.at[s], a_r.at[s, 2], at_x(1 if s == 0 else -1, c))

    def x_wait(s):
        @pl.when(away(s) == 0)
        def _():
            x_local().wait()

        @pl.when((away(s) == 1) | (away(s) == 2))
        def _():
            for q in (2, 3):
                x_arrival(s, q).wait_recv()

        @pl.when((away(s) == 3) | (away(s) == 2))
        def _():
            for q in (0, 1):
                x_arrival(s, q).wait_recv()

    def project(s, start, size):
        cols = pl.ds(start, size)
        acc[s, :, cols] = jnp.zeros((total, size), jnp.float32)

        def part_of(i, carry):
            deep = pl.ds(pl.multiple_of(i * KC, KC), KC)
            acc[s, :, cols] += jnp.dot(
                xbuf[s, :, deep], wbuf[deep, cols], preferred_element_type=jnp.float32
            )
            return carry

        lax.fori_loop(0, wbuf.shape[0] // KC, part_of, 0)

    def cache_rows(s):
        length = meta[2 * c + s, pl.ds(1, 1), :]
        keys = rotated(acc[s, :, q_cols : q_cols + HD])
        values = acc[s, :, q_cols + HD :]
        live = position < length
        kept_keys = jnp.where(live, keys, 0.0).astype(jnp.bfloat16)
        kept_values = jnp.where(live, values, 0.0).astype(jnp.bfloat16)

        @pl.when(c == 0)
        def _():
            kvall[s] = kept_keys
            swap[s] = kept_values

        @pl.when(c == 1)
        def _():
            kvall[2 + s] = kept_values
            swap[s] = kept_keys

        kvbuf[s, 0] = keys.astype(jnp.bfloat16)
        kvbuf[s, 1] = values.astype(jnp.bfloat16)

    def attend(s):
        keys, values = kvbuf[s, 0], kvbuf[s, 1]
        length = meta[2 * c + s, pl.ds(1, 1), :]
        wide = jnp.concatenate([length] * (total // HD), axis=1)
        allowed = (query_at >= key_at) & (key_at < wide)
        for g in range(groups):
            query = rotated(acc[s, :, g * HD : (g + 1) * HD]).astype(jnp.bfloat16)
            scores = lax.dot_general(
                query, keys, (((1,), (1,)), ((), ())), preferred_element_type=jnp.float32
            ) * (1.0 / math.sqrt(HD))
            scores = jnp.where(allowed, scores, -jnp.inf)
            expo = jnp.exp(scores - jnp.max(scores, axis=1, keepdims=True))
            weights = (expo / jnp.sum(expo, axis=1, keepdims=True)).astype(jnp.bfloat16)
            att[s, x, :, g * HD : (g + 1) * HD] = jnp.dot(
                weights, values, preferred_element_type=jnp.float32
            ).astype(jnp.bfloat16)
        for direction in (0, 1):
            a_send(s, direction).start()

    def swapped(s):
        return remote(swap.at[s], kvall.at[2 * c + s], swap_s.at[s], swap_r.at[s], sibling)

    def d_copy(o):
        return remote(dests.at[z], dests.at[z], dest_s.at[o], dest_r.at[o], at_z(lax.rem(z + o, nz), c))

    def c1_copy(o):
        to = lax.rem(z + o, nz)
        return remote(
            kvall.at[:, pl.ds(pl.multiple_of(to * piece, piece), piece), :],
            spread.at[pl.ds(z * NX, NX)],
            c1_s.at[o], c1_r.at[o], at_z(to, c),
        )

    def send_dest(o, carry):
        d_copy(o).start()
        return carry

    def send_c1(o, carry):
        c1_copy(o).start()
        return carry

    apart = away(0)
    near = jnp.where((apart == 1) | (apart == 2), 1, 0)
    lax.fori_loop(1, nz, send_dest, 0)
    for s in (near, 1 - near):
        x_wait(s)
        project(s, q_cols, 2 * HD)
        cache_rows(s)
        swapped(s).start()
    o_hop(0, far, last).wait_recv()
    o_sibling(far, last).start()
    o_partner(far, last).start()
    for s in (0, 1):
        swapped(s).wait_recv()
    lax.fori_loop(1, nz, send_c1, 0)
    spread[pl.ds(z * NX, NX)] = kvall[:, pl.ds(pl.multiple_of(z * piece, piece), piece), :]
    project(near, 0, q_cols)
    attend(near)
    project(1 - near, 0, q_cols)
    attend(1 - near)
    for s in (0, 1):
        a_send(s, s).wait_recv()
        a_forward(s).start()
    def d_wait(o, carry):
        d_copy(o).wait_recv()
        c1_copy(o).wait_recv()
        return carry

    lax.fori_loop(1, nz, d_wait, 0)
    all_dests = dests[...].reshape(nz, HD)
    lanes = lax.broadcasted_iota(jnp.int32, (nz, HD), 1)
    prompt = lax.broadcasted_iota(jnp.int32, (nz, HD), 0) * NX
    source = jnp.zeros((nz, HD), jnp.int32)
    for j in range(NX):
        slot = jnp.sum(jnp.where(lanes == j, all_dests, 0), axis=1, keepdims=True)
        source += jnp.where(slot == lanes, prompt + j, 0)
    srcv[...] = jnp.minimum(jnp.sum(source, axis=0, keepdims=True), NX * nz - 1)
    to_scalars = pltpu.make_async_copy(srcv, srcs, src_l)
    to_scalars.start()
    to_scalars.wait()

    def reorder(d, carry):
        perm[lax.div(d, nz), lax.rem(d, nz)] = spread[srcs[0, d]]
        return carry

    lax.fori_loop(0, NX * nz, reorder, 0)

    def c2_copy(o):
        to = lax.rem(z + o, nz)
        return remote(perm.at[:, to], heads.at[:, z], c2_s.at[o], c2_r.at[o], at_z(to, c))

    def send_c2(o, carry):
        c2_copy(o).start()
        return carry

    lax.fori_loop(1, nz, send_c2, 0)
    heads[:, z] = perm[:, z]

    def o_crossed(idx, carry):
        zs = jnp.where(
            idx == last, far,
            jnp.where(idx < half - 1, block_of(0, idx + 1), block_of(1, idx + 2 - half)),
        )
        o_part_y = o_part(zs, 1 - yb)
        remote(o_part_y, o_part_y, oy_s.at[idx], oy_r.at[idx], partner).wait_recv()
        o_y_sibling(zs, idx).start()
        return carry

    lax.fori_loop(0, last + 1, o_crossed, 0)

    def o_arrived(idx, carry):
        o_sibling(z, idx).wait_recv()
        o_y_sibling(z, idx).wait_recv()
        return carry

    lax.fori_loop(0, last + 1, o_arrived, 0)
    o_own_sibling().wait_recv()

    def head_rows(s, xs):
        core = lax.div(xs, 2)
        cols = pl.ds(pl.multiple_of(lax.rem(xs, 2) * q_cols, q_cols), q_cols)
        return lax.dot_general(
            att[s, xs], wobuf[core, :, cols], (((1,), (1,)), ((), ())),
            preferred_element_type=jnp.float32,
        )

    for s in (0, 1):
        oacc[s] = head_rows(s, x)
    for s in (0, 1):
        a_send(s, 1 - s).wait_recv()
    for s in (0, 1):
        for direction in (0, 1):
            oacc[s] += head_rows(s, lax.rem(x + (NX - 1 if direction == 0 else 1), NX))

    width = oacc.shape[2]

    def out_cols(xs):
        return pl.ds(pl.multiple_of(lax.rem(xs, 2) * width, width), width)

    def out_copy(s):
        return remote(
            obuf.at[s], out_hbm.at[:, out_cols(x)], out_s.at[s, 0], out_r.at[lax.rem(x, 2)],
            (part, (2 * c + s) * nz + z, lax.div(x, 2)),
        )

    def out_here(s):
        return pltpu.make_async_copy(obuf.at[s], out_hbm.at[:, out_cols(x)], out_l)

    def out_rows(direction):
        return pl.ds(direction * (total // 2), total // 2)

    def out_first(s, direction):
        return remote(
            obuf.at[s, out_rows(direction)], relay.at[direction], out_s.at[s, direction],
            relay_r.at[direction], at_x(1 if direction == 0 else -1, c),
        )

    def out_second(direction):
        source = lax.rem(x + (NX - 1 if direction == 0 else 1), NX)
        return remote(
            relay.at[direction], out_hbm.at[out_rows(direction), out_cols(source)],
            relay_s.at[direction], out_r.at[lax.rem(source, 2)],
            at_x(1 if direction == 0 else -1, lax.div(source, 2)),
        )

    def relays(direction):
        to = lax.rem(x + (1 if direction == 0 else NX - 1), NX)
        return lax.div(to, 2) == c

    for s in (0, 1):
        a_forward(s).wait_recv()
        obuf[s] = (oacc[s] + head_rows(s, lax.rem(x + 2, NX))).astype(jnp.bfloat16)

        @pl.when(away(s) == 2)
        def _(s=s):
            for direction in (0, 1):
                out_first(s, direction).start()

        pl.when((away(s) == 1) | (away(s) == 3))(lambda s=s: out_copy(s).start())
        pl.when(away(s) == 0)(lambda s=s: out_here(s).start())

    for direction in (0, 1):
        @pl.when(relays(direction))
        def _(direction=direction):
            out_first(0, direction).wait_recv()
            out_second(direction).start()

    def wait_c2(o, carry):
        c2_copy(o).wait_recv()
        return carry

    lax.fori_loop(1, nz, wait_c2, 0)

    def c3_copy(o, t):
        return remote(
            heads.at[lax.rem(x + o, NX), pl.ds(t * half, half)], kv_hbm.at[c, x, :, :, :],
            c3_s.at[o, t], c3_r.at[c, x], at_x(o, t),
        )

    def c3_here():
        return pltpu.make_async_copy(heads.at[x, pl.ds(c * half, half)], kv_hbm.at[c, x, :, :, :], c3_l)

    for o in range(1, NX):
        for t in (0, 1):
            c3_copy(o, t).start()
    c3_copy(0, 1 - c).start()
    c3_here().start()

    for kind in (0, 1):
        for h in range(NX):
            @pl.when((kind != c) | (h != x))
            def _(kind=kind, h=h):
                remote(
                    heads.at[0, pl.ds(0, half)], kv_hbm.at[kind, h, :, :, :],
                    c3_s.at[0, 0], c3_r.at[kind, h], sibling,
                ).wait_recv()

    c3_here().wait()
    c3_copy(0, 1 - c).wait_send()
    for o in range(1, NX):
        for t in (0, 1):
            c3_copy(o, t).wait_send()
    for i in (0, 1):
        @pl.when(2 * c + i != x)
        def _(i=i):
            cols = pl.ds(i * width, width)
            remote(obuf.at[0], out_hbm.at[:, cols], out_s.at[0, 0], out_r.at[i], sibling).wait_recv()

    for s in (0, 1):
        @pl.when(away(s) == 2)
        def _(s=s):
            for direction in (0, 1):
                out_first(s, direction).wait_send()

        pl.when((away(s) == 1) | (away(s) == 3))(lambda s=s: out_copy(s).wait_send())
        pl.when(away(s) == 0)(lambda s=s: out_here(s).wait())
        pl.when(relays(s))(lambda s=s: out_second(s).wait_send())
        for direction in (0, 1):
            a_send(s, direction).wait_send()
        a_forward(s).wait_send()
    for b in (0, 1):
        @pl.when(2 * c + b != x)
        def _(b=b):
            for copy in w0(b):
                copy.wait_send()

    for o in range(1, NX):
        meta_copy(o).wait_send()

    @pl.when(is_source)
    def _():
        for i in range(4):
            for direction in (0, 1):
                x_send(direction, i).wait_send()

    for s in (0, 1):
        for i in (0, 1):
            pl.when(away(s) == 1)(lambda s=s, i=i: x_forward(s, i, 0).wait_send())
            pl.when(away(s) == 3)(lambda s=s, i=i: x_forward(s, 2 + i, 1).wait_send())
        own_to_sibling(s).wait_send()
        swapped(s).wait_send()
    o_own_sibling().wait_send()

    def drain_z(o, carry):
        d_copy(o).wait_send()
        c1_copy(o).wait_send()
        c2_copy(o).wait_send()
        return carry

    lax.fori_loop(1, nz, drain_z, 0)

    def drain_ring(idx, carry):
        hop(0, z, idx, 0).wait_send()
        hop(0, z, idx, 1).wait_send()
        to_sibling(z, idx).wait_send()
        to_partner(z, idx).wait_send()
        y_to_sibling(z, idx).wait_send()
        o_hop(0, z, idx).wait_send()
        o_partner(z, idx).wait_send()
        o_y_sibling(z, idx).wait_send()
        o_sibling(z, idx).wait_send()
        return carry

    lax.fori_loop(0, last + 1, drain_ring, 0)


def on_device(normed, q_weight, kv_weight, o_weight, lengths, destinations):
    tokens = normed[0]
    total, width = tokens.shape
    nz = lax.axis_size("dp") // NX
    rows = q_weight.shape[0]
    q_cols = q_weight.shape[1] // 2
    kv_rows = kv_weight.reshape(rows, -1)
    o_t = o_weight.T
    cosine, sine = tables(total)
    columns = q_cols + 2 * HD
    o_cols = rows * nz
    piece = total // nz
    hops = nz - 1
    bf16, f32 = jnp.bfloat16, jnp.float32
    dma = pltpu.SemaphoreType.DMA
    scratch = [
        pltpu.VMEM((width, columns), bf16),
        pltpu.VMEM((2, o_cols, o_weight.shape[0]), bf16),
        pltpu.VMEM((2, total, width), bf16),
        pltpu.VMEM((2, NX, total, q_cols), bf16),
        pltpu.VMEM((2, total, columns), f32),
        pltpu.VMEM((2, total, o_cols), f32),
        pltpu.VMEM((2, total, o_cols), bf16),
        pltpu.VMEM((NX, 2, HD), jnp.int32),
        pltpu.VMEM((nz, 1, HD), jnp.int32),
        pltpu.VMEM((1, HD), jnp.int32),
        pltpu.SMEM((1, HD), jnp.int32),
        pltpu.VMEM((NX, total, HD), bf16),
        pltpu.VMEM((2, total, HD), bf16),
        pltpu.VMEM((NX * nz, piece, HD), bf16),
        pltpu.VMEM((NX, nz, piece, HD), bf16),
        pltpu.VMEM((NX, nz, piece, HD), bf16),
    ]
    shapes = [
        (NX,), (NX,), (2, 3), (2,), (hops, 2), (hops, 2), (hops,), (hops,), (hops,), (hops,), (hops,), (hops,), (2,), (2,),
        (hops,), (hops,), (hops,), (hops,), None, None, None, (2, 4), (2, 2), (2, 4), (2, 2), (2,), (2, 3), (2,), (2,),
        (nz,), (nz,), (nz,), (nz,), None, (nz,), (nz,), (NX, 2), (2, NX), None, (2, 2), (2,), None,
    ]
    scratch += [dma if shape is None else dma(shape) for shape in shapes]
    scratch.append(pltpu.SemaphoreType.REGULAR((2,)))
    scratch += [pltpu.VMEM((2, 2, total, HD), bf16), pltpu.VMEM((2, total // 2, o_cols), bf16), dma((2,)), dma((2,))]
    scratch += [dma((hops,))] * 4
    smem = pl.BlockSpec(memory_space=pltpu.SMEM)
    vmem = pl.BlockSpec(memory_space=pltpu.VMEM)
    any_space = pl.BlockSpec(memory_space=pl.ANY)
    projected, cache = pl.pallas_call(
        functools.partial(kernel, nz),
        out_shape=(
            jax.ShapeDtypeStruct((total, 2 * o_cols), bf16),
            jax.ShapeDtypeStruct((2, NX, nz // 2, piece, HD), bf16),
        ),
        in_specs=[any_space, vmem, vmem, vmem, vmem, vmem, smem, smem],
        out_specs=(any_space, any_space),
        scratch_shapes=scratch,
        compiler_params=pltpu.CompilerParams(
            collective_id=0, has_side_effects=True, vmem_limit_bytes=60 * 1024 * 1024
        ),
    )(tokens, q_weight, kv_rows, o_t, cosine, sine, destinations, lengths)
    return (projected[None], cache.reshape(1, 2, NX, total // 2, HD))


def solution(mesh):
    placed = (
        P(("parts", "dp"), None, None),
        P("dp", "tensor"),
        P("dp", None, "tensor"),
        P("tensor", "dp"),
        P(("parts", "dp")),
        P(("parts", "dp")),
    )
    return jax.shard_map(
        on_device,
        mesh=mesh,
        in_specs=placed,
        out_specs=(
            P(("parts", "dp"), None, "tensor"),
            P(("parts", "dp"), None, None, "tensor", None),
        ),
        check_vma=False,
    )
```

```python
import functools
import math

import jax
import jax.numpy as jnp
import numpy as np
from jax import lax
from jax.experimental import pallas as pl
from jax.experimental.pallas import tpu as pltpu
from jax.sharding import PartitionSpec as P

HD = 128
ROPE_BASE = 500000.0
NX = 4
KC = 1024
QC = 64
LAG = 1
Y_LAG = 3


def tables(total):
    half = HD // 2
    steps = np.arange(half, dtype=np.float32) * np.float32(2.0 / HD)
    freq = np.power(np.float32(ROPE_BASE), -steps)
    angle = np.arange(total, dtype=np.float32)[:, None] * freq[None, :]
    cosine, sine = np.cos(angle), np.sin(angle)
    return (
        jnp.asarray(np.concatenate([cosine, cosine], axis=-1)),
        jnp.asarray(np.concatenate([-sine, sine], axis=-1)),
    )


def remote(src, dst, send, recv, device):
    return pltpu.make_async_remote_copy(
        src_ref=src,
        dst_ref=dst,
        send_sem=send,
        recv_sem=recv,
        device_id=device,
        device_id_type=pl.DeviceIdType.MESH,
    )


def kernel(
    nz, x_hbm, q_ref, kv_ref, o_t, cos_ref, sin_ref, dest_ref, length_ref, out_hbm, kv_hbm,
    wbuf, wobuf, xbuf, att, acc, oacc, obuf, meta, dests, srcv, srcs, kvall, swap, spread, perm, heads,
    meta_s, meta_r, w0_s, w0_r, ring_s, ring_r, sib_s, sib_r, y_s, y_r, own_s, own_r,
    o_s, o_r, osib_s, osib_r, oown_s, oown_r, x_l, x_s, xf_s, x_r, a_s, af_s, a_r, swap_s, swap_r,
    dest_s, dest_r, c1_s, c1_r, src_l, c2_s, c2_r, c3_s, c3_r, c3_l, out_s, out_r, out_l, ready, kvbuf, relay, relay_s, relay_r,
    oy_s, oy_r, oysib_s, oysib_r,
):
    part, dp, c = lax.axis_index("parts"), lax.axis_index("dp"), lax.axis_index("tensor")
    x, z = lax.div(dp, nz), lax.rem(dp, nz)
    half = nz // 2
    yb = lax.rem(part, 2)
    mate = part + 1 - 2 * yb
    rows = q_ref.shape[0]
    total = xbuf.shape[1]
    piece = total // nz
    last = 2 * (half - 1)

    def at_x(offset, core):
        return (part, lax.rem(x + offset + NX, NX) * nz + z, core)

    def at_z(where, core):
        return (part, x * nz + where, core)

    sibling = (part, dp, 1 - c)
    partner = (mate, dp, c)
    up, down = lax.rem(z + 1, nz), lax.rem(z + nz - 1, nz)

    barrier = pltpu.get_barrier_semaphore()

    def greet(semaphore, device):
        pl.semaphore_signal(semaphore, inc=1, device_id=device, device_id_type=pl.DeviceIdType.MESH)

    greeted = [at_x(o, k) for o in range(1, NX) for k in (0, 1)] + [sibling, partner]
    for device in greeted:
        greet(barrier, device)
    pl.when(z != 0)(lambda: greet(barrier, at_z(up, c)))
    pl.when(z == 1)(lambda: greet(barrier, at_z(down, c)))
    pl.semaphore_wait(
        barrier, len(greeted) + jnp.where(z == 1, 0, 1) + jnp.where(z == 0, 1, 0)
    )
    pl.when(z != 1)(lambda: greet(ready.at[0], at_z(down, c)))
    pl.when(z == 0)(lambda: greet(ready.at[1], at_z(up, c)))

    columns = wbuf.shape[2]
    q_cols = columns - 2 * HD

    def w_block(xs, zs):
        return wbuf.at[xs, pl.ds(pl.multiple_of(zs * rows, rows), rows), :]

    def w0_parts(b):
        return (
            (q_ref, b * q_cols, 0, q_cols),
            (kv_ref, b * HD, q_cols, HD),
            (kv_ref, (2 + b) * HD, q_cols + HD, HD),
        )

    def w0(b):
        block = w_block(x, z)
        return [
            remote(
                src.at[:, pl.ds(start, size)], block.at[:, pl.ds(to, size)], w0_s.at[b, i],
                w0_r.at[lax.rem(x, 2)], (part, (2 * c + b) * nz + z, lax.div(x, 2)),
            )
            for i, (src, start, to, size) in enumerate(w0_parts(b))
        ]

    for b in (0, 1):
        @pl.when(2 * c + b != x)
        def _(b=b):
            for copy in w0(b):
                copy.start()

    for b in (0, 1):
        @pl.when(2 * c + b == x)
        def _(b=b):
            block = w_block(x, z)
            for src, start, to, size in w0_parts(b):
                block[:, to : to + size] = src[:, start : start + size]

    meta[x] = jnp.concatenate(
        [jnp.full((1, HD), dest_ref[0], jnp.int32), jnp.full((1, HD), length_ref[0], jnp.int32)]
    )

    def meta_copy(o):
        return remote(meta.at[x], meta.at[x], meta_s.at[o], meta_r.at[o], at_x(o, c))

    for o in range(1, NX):
        meta_copy(o).start()

    quarter = total // 4

    def away(s):
        return lax.rem(x - 2 * c - s + 2 * NX, NX)

    is_source = lax.div(x, 2) == c
    mine = lax.rem(x, 2)

    def x_rows(q):
        return pl.ds(q * quarter, quarter)

    def x_send(direction, q):
        return remote(
            x_hbm.at[x_rows(q)], xbuf.at[mine, x_rows(q)], x_s.at[direction, q], x_r.at[mine, q],
            at_x(1 if direction == 0 else -1, c),
        )

    def x_local():
        return pltpu.make_async_copy(x_hbm, xbuf.at[mine], x_l)

    def x_forward(s, q, direction):
        return remote(
            xbuf.at[s, x_rows(q)], xbuf.at[s, x_rows(q)], xf_s.at[s, q % 2], x_r.at[s, q],
            at_x(1 if direction == 0 else -1, c),
        )

    @pl.when(is_source)
    def _():
        for i in range(4):
            x_send(0, i).start()
            x_send(1, (i + 2) % 4).start()
        x_local().start()

    def x_arrival(s, q):
        rows_of = xbuf.at[s, x_rows(q)]
        return remote(rows_of, rows_of, xf_s.at[s, q % 2], x_r.at[s, q], sibling)

    def pass_on(i):
        for s in (0, 1):
            @pl.when(away(s) == 1)
            def _(s=s):
                x_forward(s, i, 0).wait_recv()
                x_forward(s, i, 0).start()

            @pl.when(away(s) == 3)
            def _(s=s):
                x_forward(s, 2 + i, 1).wait_recv()
                x_forward(s, 2 + i, 1).start()

    def w_part(zs, core, which):
        cols = pl.ds(q_cols, 2 * HD)
        if which:
            at = yb if which == 1 else 1 - yb
            cols = pl.ds(pl.multiple_of(at * (q_cols // 2), q_cols // 2), q_cols // 2)
        return wbuf.at[pl.ds(2 * core, 2), pl.ds(pl.multiple_of(zs * rows, rows), rows), cols]

    def hop(direction, zs, idx, which):
        blk = w_part(zs, c, which)
        return remote(
            blk, blk, ring_s.at[idx, which], ring_r.at[idx, which],
            at_z(up if direction == 0 else down, c),
        )

    def to_sibling(zs, idx, which):
        blk = w_part(zs, c, which)
        return remote(blk, blk, sib_s.at[idx, which], sib_r.at[idx, which], sibling)

    def to_partner(zs, idx):
        blk = w_part(zs, c, 1)
        return remote(blk, blk, y_s.at[idx], y_r.at[idx], partner)

    def from_partner(zs, idx):
        blk = w_part(zs, c, 2)
        return remote(blk, blk, y_s.at[idx], y_r.at[idx], partner)

    def own_to_sibling():
        blk = wbuf.at[pl.ds(2 * c, 2), pl.ds(pl.multiple_of(z * rows, rows), rows), :]
        return remote(blk, blk, own_s, own_r, sibling)

    def o_block(zs, core):
        return wobuf.at[core, pl.ds(pl.multiple_of(zs * QC, QC), QC), :]

    def o_part(zs, which):
        start = pl.multiple_of(zs * QC + which * (QC // 2), QC // 2)
        return wobuf.at[c, pl.ds(start, QC // 2), :]

    def o_hop(direction, zs, idx, src=None):
        blk = o_part(zs, yb)
        return remote(
            blk if src is None else src, blk, o_s.at[idx], o_r.at[idx],
            at_z(up if direction == 0 else down, c),
        )

    def o_sibling(zs, idx):
        blk = o_part(zs, yb)
        return remote(blk, blk, osib_s.at[idx], osib_r.at[idx], sibling)

    def o_partner(zs, idx):
        blk = o_part(zs, yb)
        return remote(blk, blk, oy_s.at[idx], oy_r.at[idx], partner)

    def o_y_sibling(zs, idx):
        blk = o_part(zs, 1 - yb)
        return remote(blk, blk, oysib_s.at[idx], oysib_r.at[idx], sibling)

    def o_own_sibling():
        return remote(o_t, o_block(z, c), oown_s, oown_r, sibling)

    for i in (0, 1):
        @pl.when(2 * c + i != x)
        def _(i=i):
            blk = w_block(2 * c + i, z)
            remote(blk, blk, w0_s.at[0, 0], w0_r.at[i], sibling).wait_recv()

    first = (0, half - 1)
    own_to_sibling().start()
    pl.when(z != 0)(lambda: pl.semaphore_wait(ready.at[0], 1))
    for h in (0, 1):
        hop(0, z, first[0], h).start()
    pl.when(z == 1)(lambda: pl.semaphore_wait(ready.at[1], 1))
    for h in (0, 1):
        hop(1, z, first[1], h).start()
    o_block(z, c)[...] = o_t[...]

    def block_of(direction, k):
        return lax.rem(z + (nz - k if direction == 0 else k), nz)

    def slot_of(direction, k):
        return direction * (half - 1) + k - 1

    def partner_on(direction, k, idx):
        zs = block_of(direction, k)
        from_partner(zs, idx).wait_recv()
        to_sibling(zs, idx, 2).start()

    def w_half(direction, k, h):
        idx = slot_of(direction, k)
        zs = block_of(direction, k)
        hop(direction, zs, idx, h).wait_recv()

        @pl.when((k < half - 1) | (c == direction))
        def _():
            hop(direction, zs, jnp.where(k == half - 1, last, idx + 1), h).start()

    def w_rest(direction, k):
        idx = slot_of(direction, k)
        zs = block_of(direction, k)
        to_sibling(zs, idx, 0).start()
        to_sibling(zs, idx, 1).start()
        to_partner(zs, idx).start()

    def o_step(k):
        for direction in (0, 1):
            idx = slot_of(direction, k)
            zs = block_of(direction, k)
            o_hop(direction, zs, idx).wait_recv()

            @pl.when((k < half - 1) | (c == direction))
            def _(direction=direction, idx=idx, zs=zs):
                o_hop(direction, zs, jnp.where(k == half - 1, last, idx + 1)).start()

            o_sibling(zs, idx).start()
            if direction == 0:
                o_partner(zs, idx).start()

    def ring_step(k, carry):
        for h in (0, 1):
            for direction in (0, 1):
                w_half(direction, k, h)
        for direction in (0, 1):
            w_rest(direction, k)
        @pl.when(k > LAG)
        def _():
            o_step(k - LAG)

        @pl.when(k > Y_LAG)
        def _():
            for direction in (0, 1):
                partner_on(direction, k - Y_LAG, slot_of(direction, k - Y_LAG))

        return carry

    for direction in (0, 1):
        o_hop(direction, z, first[direction], o_t.at[pl.ds(pl.multiple_of(yb * (QC // 2), QC // 2), QC // 2)]).start()
    o_own_sibling().start()
    lax.fori_loop(1, 3, ring_step, 0)
    pass_on(0)
    lax.fori_loop(3, 5, ring_step, 0)
    pass_on(1)
    lax.fori_loop(5, half, ring_step, 0)
    far = block_of(0, half)
    for which in (0, 1):
        hop(0, far, last, which).wait_recv()
        to_sibling(far, last, which).start()
    to_partner(far, last).start()

    def arrived(idx, carry):
        to_sibling(z, idx, 0).wait_recv()
        return carry

    lax.fori_loop(0, last + 1, arrived, 0)
    own_to_sibling().wait_recv()
    for o in range(1, NX):
        meta_copy(o).wait_recv()

    lane = lax.broadcasted_iota(jnp.int32, (1, HD), 1)
    row = jnp.zeros((1, HD), jnp.int32)
    for j in range(NX):
        row = jnp.where(lane == j, meta[j, pl.ds(0, 1), :], row)
    dests[z] = row

    cosine, sine = cos_ref[...], sin_ref[...]

    def rotated(u):
        return u * cosine + pltpu.roll(u, HD // 2, 1) * sine

    groups = q_cols // HD
    key_at = lax.broadcasted_iota(jnp.int32, (total, total), 1)
    query_at = lax.broadcasted_iota(jnp.int32, (total, total), 0)
    position = lax.broadcasted_iota(jnp.int32, (total, HD), 0)

    def a_send(s, direction):
        return remote(
            att.at[s, x], att.at[s, x], a_s.at[s, direction], a_r.at[s, direction],
            at_x(1 if direction == 0 else -1, c),
        )

    def a_forward(s, direction):
        source = lax.rem(x + (NX - 1 if direction == 0 else 1), NX)
        blk = att.at[s, source, pl.ds(direction * (total // 2), total // 2)]
        return remote(
            blk, blk, af_s.at[s, direction], a_r.at[s, 2 + direction],
            at_x(1 if direction == 0 else -1, c),
        )

    def pass_attended(s):
        for direction in (0, 1):
            a_send(s, direction).wait_recv()
        for direction in (0, 1):
            a_forward(s, direction).start()

    def x_wait(s):
        @pl.when(away(s) == 0)
        def _():
            x_local().wait()

        @pl.when((away(s) == 1) | (away(s) == 2))
        def _():
            for q in (2, 3):
                x_arrival(s, q).wait_recv()

        @pl.when((away(s) == 3) | (away(s) == 2))
        def _():
            for q in (0, 1):
                x_arrival(s, q).wait_recv()

    def project(start, size):
        cols = pl.ds(start, size)
        per = nz * rows // KC

        def part_of(i):
            deep = pl.ds(pl.multiple_of(i * KC, KC), KC)
            inside = pl.ds(pl.multiple_of(lax.rem(i, per) * KC, KC), KC)
            both = xbuf[:, :, deep].reshape(2 * total, KC)
            return jnp.dot(
                both, wbuf[lax.div(i, per), inside, cols], preferred_element_type=jnp.float32
            ).reshape(2, total, size)

        acc[:, :, cols] = part_of(0)

        def add(i, carry):
            acc[:, :, cols] += part_of(i)
            return carry

        lax.fori_loop(1, xbuf.shape[2] // KC, add, 0)

    def cache_rows(s):
        length = meta[2 * c + s, pl.ds(1, 1), :]
        keys = rotated(acc[s, :, q_cols : q_cols + HD])
        values = acc[s, :, q_cols + HD :]
        live = position < length
        kept_keys = jnp.where(live, keys, 0.0).astype(jnp.bfloat16)
        kept_values = jnp.where(live, values, 0.0).astype(jnp.bfloat16)

        @pl.when(c == 0)
        def _():
            kvall[s] = kept_keys
            swap[s] = kept_values

        @pl.when(c == 1)
        def _():
            kvall[2 + s] = kept_values
            swap[s] = kept_keys

        kvbuf[s, 0] = keys.astype(jnp.bfloat16)
        kvbuf[s, 1] = values.astype(jnp.bfloat16)

    def attend(s):
        keys, values = kvbuf[s, 0], kvbuf[s, 1]
        length = meta[2 * c + s, pl.ds(1, 1), :]
        wide = jnp.concatenate([length] * (total // HD), axis=1)
        allowed = (query_at >= key_at) & (key_at < wide)
        for g in range(groups):
            query = rotated(acc[s, :, g * HD : (g + 1) * HD]).astype(jnp.bfloat16)
            scores = lax.dot_general(
                query, keys, (((1,), (1,)), ((), ())), preferred_element_type=jnp.float32
            ) * (1.0 / math.sqrt(HD))
            scores = jnp.where(allowed, scores, -jnp.inf)
            expo = jnp.exp(scores - jnp.max(scores, axis=1, keepdims=True))
            weights = (expo / jnp.sum(expo, axis=1, keepdims=True)).astype(jnp.bfloat16)
            att[s, x, :, g * HD : (g + 1) * HD] = jnp.dot(
                weights, values, preferred_element_type=jnp.float32
            ).astype(jnp.bfloat16)
        for direction in (0, 1):
            a_send(s, direction).start()

    def swapped(s):
        return remote(swap.at[s], kvall.at[2 * c + s], swap_s.at[s], swap_r.at[s], sibling)

    def d_copy(o):
        return remote(dests.at[z], dests.at[z], dest_s.at[o], dest_r.at[o], at_z(lax.rem(z + o, nz), c))

    def c1_copy(o):
        to = lax.rem(z + o, nz)
        return remote(
            kvall.at[:, pl.ds(pl.multiple_of(to * piece, piece), piece), :],
            spread.at[pl.ds(z * NX, NX)],
            c1_s.at[o], c1_r.at[o], at_z(to, c),
        )

    def send_dest(o, carry):
        d_copy(o).start()
        return carry

    def send_c1(o, carry):
        c1_copy(o).start()
        return carry

    lax.fori_loop(1, nz, send_dest, 0)
    for s in (0, 1):
        x_wait(s)
    project(q_cols, 2 * HD)
    for s in (0, 1):
        cache_rows(s)
        swapped(s).start()
    for k in range(half - LAG, half):
        o_step(k)
    def o_over(k, carry):
        o_partner(block_of(1, k), slot_of(1, k)).start()
        return carry

    lax.fori_loop(1, half, o_over, 0)

    for k in range(half - Y_LAG, half):
        for direction in (0, 1):
            partner_on(direction, k, slot_of(direction, k))
    partner_on(0, half, last)
    for s in (0, 1):
        swapped(s).wait_recv()
    lax.fori_loop(1, nz, send_c1, 0)
    spread[pl.ds(z * NX, NX)] = kvall[:, pl.ds(pl.multiple_of(z * piece, piece), piece), :]
    def q_arrived(idx, carry):
        to_sibling(z, idx, 1).wait_recv()
        to_sibling(z, idx, 2).wait_recv()
        return carry

    lax.fori_loop(0, last + 1, q_arrived, 0)
    project(0, q_cols)
    o_hop(0, far, last).wait_recv()
    o_sibling(far, last).start()
    o_partner(far, last).start()
    attend(0)
    attend(1)
    pass_attended(0)
    def d_wait(o, carry):
        d_copy(o).wait_recv()
        c1_copy(o).wait_recv()
        return carry

    lax.fori_loop(1, nz, d_wait, 0)
    all_dests = dests[...].reshape(nz, HD)
    lanes = lax.broadcasted_iota(jnp.int32, (nz, HD), 1)
    prompt = lax.broadcasted_iota(jnp.int32, (nz, HD), 0) * NX
    source = jnp.zeros((nz, HD), jnp.int32)
    for j in range(NX):
        slot = jnp.sum(jnp.where(lanes == j, all_dests, 0), axis=1, keepdims=True)
        source += jnp.where(slot == lanes, prompt + j, 0)
    srcv[...] = jnp.minimum(jnp.sum(source, axis=0, keepdims=True), NX * nz - 1)
    to_scalars = pltpu.make_async_copy(srcv, srcs, src_l)
    to_scalars.start()
    to_scalars.wait()

    def reorder(d, carry):
        for j in range(NX):
            perm[j, d] = spread[srcs[0, j * nz + d]]
        return carry

    lax.fori_loop(0, nz, reorder, 0, unroll=4)

    def c2_copy(o):
        to = lax.rem(z + o, nz)
        return remote(perm.at[:, to], heads.at[:, z], c2_s.at[o], c2_r.at[o], at_z(to, c))

    def send_c2(o, carry):
        c2_copy(o).start()
        return carry

    lax.fori_loop(1, nz, send_c2, 0)
    heads[:, z] = perm[:, z]
    def o_crossed(idx, carry):
        zs = jnp.where(
            idx == last, far,
            jnp.where(idx < half - 1, block_of(0, idx + 1), block_of(1, idx + 2 - half)),
        )
        o_part_y = o_part(zs, 1 - yb)
        remote(o_part_y, o_part_y, oy_s.at[idx], oy_r.at[idx], partner).wait_recv()
        o_y_sibling(zs, idx).start()
        return carry

    lax.fori_loop(0, last + 1, o_crossed, 0)

    pass_attended(1)
    def o_arrived(idx, carry):
        o_sibling(z, idx).wait_recv()
        o_y_sibling(z, idx).wait_recv()
        return carry

    lax.fori_loop(0, last + 1, o_arrived, 0)
    o_own_sibling().wait_recv()

    def head_rows(s, xs):
        core = lax.div(xs, 2)
        cols = pl.ds(pl.multiple_of(lax.rem(xs, 2) * q_cols, q_cols), q_cols)
        return lax.dot_general(
            att[s, xs], wobuf[core, :, cols], (((1,), (1,)), ((), ())),
            preferred_element_type=jnp.float32,
        )

    for s in (0, 1):
        oacc[s] = head_rows(s, x)
        for direction in (0, 1):
            oacc[s] += head_rows(s, lax.rem(x + (NX - 1 if direction == 0 else 1), NX))

    width = oacc.shape[2]

    def out_cols(xs):
        return pl.ds(pl.multiple_of(lax.rem(xs, 2) * width, width), width)

    def out_copy(s):
        return remote(
            obuf.at[s], out_hbm.at[:, out_cols(x)], out_s.at[s, 0], out_r.at[lax.rem(x, 2)],
            (part, (2 * c + s) * nz + z, lax.div(x, 2)),
        )

    def out_here(s):
        return pltpu.make_async_copy(obuf.at[s], out_hbm.at[:, out_cols(x)], out_l)

    def out_rows(direction):
        return pl.ds(direction * (total // 2), total // 2)

    def out_first(s, direction):
        return remote(
            obuf.at[s, out_rows(direction)], relay.at[direction], out_s.at[s, direction],
            relay_r.at[direction], at_x(1 if direction == 0 else -1, c),
        )

    def out_second(direction):
        source = lax.rem(x + (NX - 1 if direction == 0 else 1), NX)
        return remote(
            relay.at[direction], out_hbm.at[out_rows(direction), out_cols(source)],
            relay_s.at[direction], out_r.at[lax.rem(source, 2)],
            at_x(1 if direction == 0 else -1, lax.div(source, 2)),
        )

    def relays(direction):
        to = lax.rem(x + (1 if direction == 0 else NX - 1), NX)
        return lax.div(to, 2) == c

    for s in (0, 1):
        for direction in (0, 1):
            a_forward(s, direction).wait_recv()
        obuf[s] = (oacc[s] + head_rows(s, lax.rem(x + 2, NX))).astype(jnp.bfloat16)

        @pl.when(away(s) == 2)
        def _(s=s):
            for direction in (0, 1):
                out_first(s, direction).start()

        pl.when((away(s) == 1) | (away(s) == 3))(lambda s=s: out_copy(s).start())
        pl.when(away(s) == 0)(lambda s=s: out_here(s).start())

    for direction in (0, 1):
        @pl.when(relays(direction))
        def _(direction=direction):
            out_first(0, direction).wait_recv()
            out_second(direction).start()

    def wait_c2(o, carry):
        c2_copy(o).wait_recv()
        return carry

    lax.fori_loop(1, nz, wait_c2, 0)

    def c3_copy(o, t):
        return remote(
            heads.at[lax.rem(x + o, NX), pl.ds(t * half, half)], kv_hbm.at[c, x, :, :, :],
            c3_s.at[o, t], c3_r.at[c, x], at_x(o, t),
        )

    def c3_here():
        return pltpu.make_async_copy(heads.at[x, pl.ds(c * half, half)], kv_hbm.at[c, x, :, :, :], c3_l)

    for o in range(1, NX):
        for t in (0, 1):
            c3_copy(o, t).start()
    c3_copy(0, 1 - c).start()
    c3_here().start()

    for kind in (0, 1):
        for h in range(NX):
            @pl.when((kind != c) | (h != x))
            def _(kind=kind, h=h):
                remote(
                    heads.at[0, pl.ds(0, half)], kv_hbm.at[kind, h, :, :, :],
                    c3_s.at[0, 0], c3_r.at[kind, h], sibling,
                ).wait_recv()

    c3_here().wait()
    c3_copy(0, 1 - c).wait_send()
    for o in range(1, NX):
        for t in (0, 1):
            c3_copy(o, t).wait_send()
    for i in (0, 1):
        @pl.when(2 * c + i != x)
        def _(i=i):
            cols = pl.ds(i * width, width)
            remote(obuf.at[0], out_hbm.at[:, cols], out_s.at[0, 0], out_r.at[i], sibling).wait_recv()

    for s in (0, 1):
        @pl.when(away(s) == 2)
        def _(s=s):
            for direction in (0, 1):
                out_first(s, direction).wait_send()

        pl.when((away(s) == 1) | (away(s) == 3))(lambda s=s: out_copy(s).wait_send())
        pl.when(away(s) == 0)(lambda s=s: out_here(s).wait())
        pl.when(relays(s))(lambda s=s: out_second(s).wait_send())
        for direction in (0, 1):
            a_send(s, direction).wait_send()
        for direction in (0, 1):
            a_forward(s, direction).wait_send()
    for b in (0, 1):
        @pl.when(2 * c + b != x)
        def _(b=b):
            for copy in w0(b):
                copy.wait_send()

    for o in range(1, NX):
        meta_copy(o).wait_send()

    @pl.when(is_source)
    def _():
        for i in range(4):
            for direction in (0, 1):
                x_send(direction, i).wait_send()

    for s in (0, 1):
        for i in (0, 1):
            pl.when(away(s) == 1)(lambda s=s, i=i: x_forward(s, i, 0).wait_send())
            pl.when(away(s) == 3)(lambda s=s, i=i: x_forward(s, 2 + i, 1).wait_send())
        swapped(s).wait_send()
    own_to_sibling().wait_send()
    o_own_sibling().wait_send()

    def drain_z(o, carry):
        d_copy(o).wait_send()
        c1_copy(o).wait_send()
        c2_copy(o).wait_send()
        return carry

    lax.fori_loop(1, nz, drain_z, 0)

    def drain_ring(idx, carry):
        hop(0, z, idx, 0).wait_send()
        hop(0, z, idx, 1).wait_send()
        for which in (0, 1, 2):
            to_sibling(z, idx, which).wait_send()
        to_partner(z, idx).wait_send()
        o_hop(0, z, idx).wait_send()
        o_partner(z, idx).wait_send()
        o_y_sibling(z, idx).wait_send()
        o_sibling(z, idx).wait_send()
        return carry

    lax.fori_loop(0, last + 1, drain_ring, 0)


def on_device(normed, q_weight, kv_weight, o_weight, lengths, destinations):
    tokens = normed[0]
    total, width = tokens.shape
    nz = lax.axis_size("dp") // NX
    rows = q_weight.shape[0]
    q_cols = q_weight.shape[1] // 2
    kv_rows = kv_weight.reshape(rows, -1)
    o_t = o_weight.T
    cosine, sine = tables(total)
    columns = q_cols + 2 * HD
    o_cols = rows * nz
    piece = total // nz
    hops = nz - 1
    bf16, f32 = jnp.bfloat16, jnp.float32
    dma = pltpu.SemaphoreType.DMA
    scratch = [
        pltpu.VMEM((NX, width // NX, columns), bf16),
        pltpu.VMEM((2, o_cols, o_weight.shape[0]), bf16),
        pltpu.VMEM((2, total, width), bf16),
        pltpu.VMEM((2, NX, total, q_cols), bf16),
        pltpu.VMEM((2, total, columns), f32),
        pltpu.VMEM((2, total, o_cols), f32),
        pltpu.VMEM((2, total, o_cols), bf16),
        pltpu.VMEM((NX, 2, HD), jnp.int32),
        pltpu.VMEM((nz, 1, HD), jnp.int32),
        pltpu.VMEM((1, HD), jnp.int32),
        pltpu.SMEM((1, HD), jnp.int32),
        pltpu.VMEM((NX, total, HD), bf16),
        pltpu.VMEM((2, total, HD), bf16),
        pltpu.VMEM((NX * nz, piece, HD), bf16),
        pltpu.VMEM((NX, nz, piece, HD), bf16),
        pltpu.VMEM((NX, nz, piece, HD), bf16),
    ]
    shapes = [
        (NX,), (NX,), (2, 3), (2,), (hops, 2), (hops, 2), (hops, 3), (hops, 3), (hops,), (hops,), None, None,
        (hops,), (hops,), (hops,), (hops,), None, None, None, (2, 4), (2, 2), (2, 4), (2, 2), (2, 2), (2, 4), (2,), (2,),
        (nz,), (nz,), (nz,), (nz,), None, (nz,), (nz,), (NX, 2), (2, NX), None, (2, 2), (2,), None,
    ]
    scratch += [dma if shape is None else dma(shape) for shape in shapes]
    scratch.append(pltpu.SemaphoreType.REGULAR((2,)))
    scratch += [pltpu.VMEM((2, 2, total, HD), bf16), pltpu.VMEM((2, total // 2, o_cols), bf16), dma((2,)), dma((2,))]
    scratch += [dma((hops,))] * 4
    smem = pl.BlockSpec(memory_space=pltpu.SMEM)
    vmem = pl.BlockSpec(memory_space=pltpu.VMEM)
    any_space = pl.BlockSpec(memory_space=pl.ANY)
    projected, cache = pl.pallas_call(
        functools.partial(kernel, nz),
        out_shape=(
            pltpu.VMEM((total, 2 * o_cols), bf16),
            pltpu.VMEM((2, NX, nz // 2, piece, HD), bf16),
        ),
        in_specs=[any_space, vmem, vmem, vmem, vmem, vmem, smem, smem],
        out_specs=(vmem, vmem),
        scratch_shapes=scratch,
        compiler_params=pltpu.CompilerParams(
            collective_id=0, has_side_effects=True, vmem_limit_bytes=60 * 1024 * 1024
        ),
    )(tokens, q_weight, kv_rows, o_t, cosine, sine, destinations, lengths)
    return (projected[None], cache.reshape(1, 2, NX, total // 2, HD))


def solution(mesh):
    placed = (
        P(("parts", "dp"), None, None),
        P("dp", "tensor"),
        P("dp", None, "tensor"),
        P("tensor", "dp"),
        P(("parts", "dp")),
        P(("parts", "dp")),
    )
    return jax.shard_map(
        on_device,
        mesh=mesh,
        in_specs=placed,
        out_specs=(
            P(("parts", "dp"), None, "tensor"),
            P(("parts", "dp"), None, None, "tensor", None),
        ),
        check_vma=False,
    )
```

```python
import functools
import math

import jax
import jax.numpy as jnp
import numpy as np
from jax import lax
from jax.experimental import pallas as pl
from jax.experimental.pallas import tpu as pltpu
from jax.sharding import PartitionSpec as P

HD = 128
ROPE_BASE = 500000.0
NX = 4
KC = 1024
QC = 64
LAG = 1
Y_LAG = 3


def tables(total):
    half = HD // 2
    steps = np.arange(half, dtype=np.float32) * np.float32(2.0 / HD)
    freq = np.power(np.float32(ROPE_BASE), -steps)
    angle = np.arange(total, dtype=np.float32)[:, None] * freq[None, :]
    cosine, sine = np.cos(angle), np.sin(angle)
    return (
        jnp.asarray(np.concatenate([cosine, cosine], axis=-1)),
        jnp.asarray(np.concatenate([-sine, sine], axis=-1)),
    )


def remote(src, dst, send, recv, device):
    return pltpu.make_async_remote_copy(
        src_ref=src,
        dst_ref=dst,
        send_sem=send,
        recv_sem=recv,
        device_id=device,
        device_id_type=pl.DeviceIdType.MESH,
    )


def kernel(
    nz, x_hbm, q_hbm, kv_rows, o_hbm, cos_hbm, sin_hbm, dest_ref, length_ref, out_hbm, kv_hbm,
    wbuf, wobuf, xbuf, att, acc, oacc, obuf, meta, dests, srcv, srcs, kvall, swap, spread, perm, heads,
    meta_s, meta_r, w0_s, w0_r, ring_s, ring_r, sib_s, sib_r, y_s, y_r, own_s, own_r,
    o_s, o_r, osib_s, osib_r, oown_s, oown_r, x_l, x_s, xf_s, x_r, a_s, af_s, a_r, swap_s, swap_r,
    dest_s, dest_r, c1_s, c1_r, src_l, c2_s, c2_r, c3_s, c3_r, c3_l, out_s, out_r, out_l, ready, kvbuf, relay, relay_s, relay_r,
    oy_s, oy_r, oysib_s, oysib_r, q_ref, kv_ref, o_t, cos_ref, sin_ref, load,
):
    part, dp, c = lax.axis_index("parts"), lax.axis_index("dp"), lax.axis_index("tensor")
    x, z = lax.div(dp, nz), lax.rem(dp, nz)
    half = nz // 2
    yb = lax.rem(part, 2)
    mate = part + 1 - 2 * yb
    rows = q_ref.shape[0]
    total = xbuf.shape[1]
    piece = total // nz
    last = 2 * (half - 1)

    def at_x(offset, core):
        return (part, lax.rem(x + offset + NX, NX) * nz + z, core)

    def at_z(where, core):
        return (part, x * nz + where, core)

    sibling = (part, dp, 1 - c)
    partner = (mate, dp, c)
    up, down = lax.rem(z + 1, nz), lax.rem(z + nz - 1, nz)

    loads = [
        pltpu.make_async_copy(src, dst, load.at[i])
        for i, (src, dst) in enumerate(
            ((q_hbm, q_ref), (kv_rows, kv_ref), (o_hbm, o_t), (cos_hbm, cos_ref), (sin_hbm, sin_ref))
        )
    ]
    for copy in loads:
        copy.start()

    barrier = pltpu.get_barrier_semaphore()

    def greet(semaphore, device):
        pl.semaphore_signal(semaphore, inc=1, device_id=device, device_id_type=pl.DeviceIdType.MESH)

    greeted = [at_x(o, k) for o in range(1, NX) for k in (0, 1)] + [sibling, partner]
    for device in greeted:
        greet(barrier, device)
    pl.when(z != 0)(lambda: greet(barrier, at_z(up, c)))
    pl.when(z == 1)(lambda: greet(barrier, at_z(down, c)))
    pl.semaphore_wait(
        barrier, len(greeted) + jnp.where(z == 1, 0, 1) + jnp.where(z == 0, 1, 0)
    )
    pl.when(z != 1)(lambda: greet(ready.at[0], at_z(down, c)))
    for copy in loads:
        copy.wait()
    pl.when(z == 0)(lambda: greet(ready.at[1], at_z(up, c)))

    columns = wbuf.shape[2]
    q_cols = columns - 2 * HD

    def w_block(xs, zs):
        return wbuf.at[xs, pl.ds(pl.multiple_of(zs * rows, rows), rows), :]

    def w0_parts(b):
        return (
            (q_ref, b * q_cols, 0, q_cols),
            (kv_ref, b * HD, q_cols, HD),
            (kv_ref, (2 + b) * HD, q_cols + HD, HD),
        )

    def w0(b):
        block = w_block(x, z)
        return [
            remote(
                src.at[:, pl.ds(start, size)], block.at[:, pl.ds(to, size)], w0_s.at[b, i],
                w0_r.at[lax.rem(x, 2)], (part, (2 * c + b) * nz + z, lax.div(x, 2)),
            )
            for i, (src, start, to, size) in enumerate(w0_parts(b))
        ]

    for b in (0, 1):
        @pl.when(2 * c + b != x)
        def _(b=b):
            for copy in w0(b):
                copy.start()

    for b in (0, 1):
        @pl.when(2 * c + b == x)
        def _(b=b):
            block = w_block(x, z)
            for src, start, to, size in w0_parts(b):
                block[:, to : to + size] = src[:, start : start + size]

    meta[x] = jnp.concatenate(
        [jnp.full((1, HD), dest_ref[0], jnp.int32), jnp.full((1, HD), length_ref[0], jnp.int32)]
    )

    def meta_copy(o):
        return remote(meta.at[x], meta.at[x], meta_s.at[o], meta_r.at[o], at_x(o, c))

    for o in range(1, NX):
        meta_copy(o).start()

    quarter = total // 4

    def away(s):
        return lax.rem(x - 2 * c - s + 2 * NX, NX)

    is_source = lax.div(x, 2) == c
    mine = lax.rem(x, 2)

    def x_rows(q):
        return pl.ds(q * quarter, quarter)

    def x_send(direction, q):
        return remote(
            x_hbm.at[x_rows(q)], xbuf.at[mine, x_rows(q)], x_s.at[direction, q], x_r.at[mine, q],
            at_x(1 if direction == 0 else -1, c),
        )

    def x_local():
        return pltpu.make_async_copy(x_hbm, xbuf.at[mine], x_l)

    def x_forward(s, q, direction):
        return remote(
            xbuf.at[s, x_rows(q)], xbuf.at[s, x_rows(q)], xf_s.at[s, q % 2], x_r.at[s, q],
            at_x(1 if direction == 0 else -1, c),
        )

    @pl.when(is_source)
    def _():
        for i in range(4):
            x_send(0, i).start()
            x_send(1, (i + 2) % 4).start()
        x_local().start()

    def x_arrival(s, q):
        rows_of = xbuf.at[s, x_rows(q)]
        return remote(rows_of, rows_of, xf_s.at[s, q % 2], x_r.at[s, q], sibling)

    def pass_on(i):
        for s in (0, 1):
            @pl.when(away(s) == 1)
            def _(s=s):
                x_forward(s, i, 0).wait_recv()
                x_forward(s, i, 0).start()

            @pl.when(away(s) == 3)
            def _(s=s):
                x_forward(s, 2 + i, 1).wait_recv()
                x_forward(s, 2 + i, 1).start()

    def w_part(zs, core, which):
        cols = pl.ds(q_cols, 2 * HD)
        if which:
            at = yb if which == 1 else 1 - yb
            cols = pl.ds(pl.multiple_of(at * (q_cols // 2), q_cols // 2), q_cols // 2)
        return wbuf.at[pl.ds(2 * core, 2), pl.ds(pl.multiple_of(zs * rows, rows), rows), cols]

    def hop(direction, zs, idx, which):
        blk = w_part(zs, c, which)
        return remote(
            blk, blk, ring_s, ring_r.at[idx, which],
            at_z(up if direction == 0 else down, c),
        )

    def to_sibling(zs, idx, which):
        blk = w_part(zs, c, which)
        return remote(blk, blk, sib_s, sib_r.at[which], sibling)

    def to_partner(zs, idx):
        blk = w_part(zs, c, 1)
        return remote(blk, blk, y_s, y_r.at[idx], partner)

    def from_partner(zs, idx):
        blk = w_part(zs, c, 2)
        return remote(blk, blk, y_s, y_r.at[idx], partner)

    def own_to_sibling():
        blk = wbuf.at[pl.ds(2 * c, 2), pl.ds(pl.multiple_of(z * rows, rows), rows), :]
        return remote(blk, blk, own_s, own_r, sibling)

    def o_block(zs, core):
        return wobuf.at[core, pl.ds(pl.multiple_of(zs * QC, QC), QC), :]

    def o_part(zs, which):
        start = pl.multiple_of(zs * QC + which * (QC // 2), QC // 2)
        return wobuf.at[c, pl.ds(start, QC // 2), :]

    def o_hop(direction, zs, idx, src=None):
        blk = o_part(zs, yb)
        return remote(
            blk if src is None else src, blk, o_s, o_r.at[idx],
            at_z(up if direction == 0 else down, c),
        )

    def o_sibling(zs, idx):
        blk = o_part(zs, yb)
        return remote(blk, blk, osib_s, osib_r, sibling)

    def o_partner(zs, idx):
        blk = o_part(zs, yb)
        return remote(blk, blk, oy_s, oy_r, partner)

    def o_y_sibling(zs, idx):
        blk = o_part(zs, 1 - yb)
        return remote(blk, blk, oysib_s, oysib_r, sibling)

    def o_own_sibling():
        return remote(o_t, o_block(z, c), oown_s, oown_r, sibling)

    for i in (0, 1):
        @pl.when(2 * c + i != x)
        def _(i=i):
            blk = w_block(2 * c + i, z)
            remote(blk, blk, w0_s.at[0, 0], w0_r.at[i], sibling).wait_recv()

    first = (0, half - 1)
    own_to_sibling().start()
    pl.when(z != 0)(lambda: pl.semaphore_wait(ready.at[0], 1))
    for h in (0, 1):
        hop(0, z, first[0], h).start()
    pl.when(z == 1)(lambda: pl.semaphore_wait(ready.at[1], 1))
    for h in (0, 1):
        hop(1, z, first[1], h).start()
    o_block(z, c)[...] = o_t[...]

    def block_of(direction, k):
        return lax.rem(z + (nz - k if direction == 0 else k), nz)

    def slot_of(direction, k):
        return direction * (half - 1) + k - 1

    def partner_on(direction, k, idx):
        zs = block_of(direction, k)
        from_partner(zs, idx).wait_recv()
        to_sibling(zs, idx, 2).start()

    def w_half(direction, k, h):
        idx = slot_of(direction, k)
        zs = block_of(direction, k)
        hop(direction, zs, idx, h).wait_recv()

        @pl.when((k < half - 1) | (c == direction))
        def _():
            hop(direction, zs, jnp.where(k == half - 1, last, idx + 1), h).start()

    def w_rest(direction, k):
        idx = slot_of(direction, k)
        zs = block_of(direction, k)
        to_sibling(zs, idx, 0).start()
        to_sibling(zs, idx, 1).start()
        to_partner(zs, idx).start()

    def o_step(k):
        for direction in (0, 1):
            idx = slot_of(direction, k)
            zs = block_of(direction, k)
            o_hop(direction, zs, idx).wait_recv()

            @pl.when((k < half - 1) | (c == direction))
            def _(direction=direction, idx=idx, zs=zs):
                o_hop(direction, zs, jnp.where(k == half - 1, last, idx + 1)).start()

            o_sibling(zs, idx).start()
            if direction == 0:
                o_partner(zs, idx).start()

    def ring_step(k, carry):
        for h in (0, 1):
            for direction in (0, 1):
                w_half(direction, k, h)
        for direction in (0, 1):
            w_rest(direction, k)
        @pl.when(k > LAG)
        def _():
            o_step(k - LAG)

        @pl.when(k > Y_LAG)
        def _():
            for direction in (0, 1):
                partner_on(direction, k - Y_LAG, slot_of(direction, k - Y_LAG))

        return carry

    for direction in (0, 1):
        o_hop(direction, z, first[direction], o_t.at[pl.ds(pl.multiple_of(yb * (QC // 2), QC // 2), QC // 2)]).start()
    o_own_sibling().start()
    lax.fori_loop(1, 3, ring_step, 0)
    pass_on(0)
    lax.fori_loop(3, 5, ring_step, 0)
    pass_on(1)
    lax.fori_loop(5, half, ring_step, 0)
    far = block_of(0, half)
    for which in (0, 1):
        hop(0, far, last, which).wait_recv()
        to_sibling(far, last, which).start()
    to_partner(far, last).start()

    def w_all(start, size, semaphores):
        blk = wbuf.at[pl.ds(0, 2), pl.ds(0, (nz - 1) * rows), pl.ds(start, size)]
        return remote(blk, blk, *semaphores, sibling)

    w_all(q_cols, 2 * HD, (sib_s, sib_r.at[0])).wait_recv()
    own_to_sibling().wait_recv()
    for o in range(1, NX):
        meta_copy(o).wait_recv()

    lane = lax.broadcasted_iota(jnp.int32, (1, HD), 1)
    row = jnp.zeros((1, HD), jnp.int32)
    for j in range(NX):
        row = jnp.where(lane == j, meta[j, pl.ds(0, 1), :], row)
    dests[z] = row

    cosine, sine = cos_ref[...], sin_ref[...]

    def rotated(u):
        return u * cosine + pltpu.roll(u, HD // 2, 1) * sine

    groups = q_cols // HD
    key_at = lax.broadcasted_iota(jnp.int32, (total, total), 1)
    query_at = lax.broadcasted_iota(jnp.int32, (total, total), 0)
    position = lax.broadcasted_iota(jnp.int32, (total, HD), 0)

    def a_send(s, direction):
        return remote(
            att.at[s, x], att.at[s, x], a_s.at[s, direction], a_r.at[s, direction],
            at_x(1 if direction == 0 else -1, c),
        )

    def a_forward(s, direction):
        source = lax.rem(x + (NX - 1 if direction == 0 else 1), NX)
        blk = att.at[s, source, pl.ds(direction * (total // 2), total // 2)]
        return remote(
            blk, blk, af_s.at[s, direction], a_r.at[s, 2 + direction],
            at_x(1 if direction == 0 else -1, c),
        )

    def pass_attended(s):
        for direction in (0, 1):
            a_send(s, direction).wait_recv()
        for direction in (0, 1):
            a_forward(s, direction).start()

    def x_wait(s):
        @pl.when(away(s) == 0)
        def _():
            x_local().wait()

        @pl.when((away(s) == 1) | (away(s) == 2))
        def _():
            for q in (2, 3):
                x_arrival(s, q).wait_recv()

        @pl.when((away(s) == 3) | (away(s) == 2))
        def _():
            for q in (0, 1):
                x_arrival(s, q).wait_recv()

    def project(start, size):
        cols = pl.ds(start, size)
        per = nz * rows // KC

        def part_of(i):
            deep = pl.ds(pl.multiple_of(i * KC, KC), KC)
            inside = pl.ds(pl.multiple_of(lax.rem(i, per) * KC, KC), KC)
            both = xbuf[:, :, deep].reshape(2 * total, KC)
            return jnp.dot(
                both, wbuf[lax.div(i, per), inside, cols], preferred_element_type=jnp.float32
            ).reshape(2, total, size)

        acc[:, :, cols] = part_of(0)

        def add(i, carry):
            acc[:, :, cols] += part_of(i)
            return carry

        lax.fori_loop(1, xbuf.shape[2] // KC, add, 0)

    def cache_rows(s):
        length = meta[2 * c + s, pl.ds(1, 1), :]
        keys = rotated(acc[s, :, q_cols : q_cols + HD])
        values = acc[s, :, q_cols + HD :]
        live = position < length
        kept_keys = jnp.where(live, keys, 0.0).astype(jnp.bfloat16)
        kept_values = jnp.where(live, values, 0.0).astype(jnp.bfloat16)

        @pl.when(c == 0)
        def _():
            kvall[s] = kept_keys
            swap[s] = kept_values

        @pl.when(c == 1)
        def _():
            kvall[2 + s] = kept_values
            swap[s] = kept_keys

        kvbuf[s, 0] = keys.astype(jnp.bfloat16)
        kvbuf[s, 1] = values.astype(jnp.bfloat16)

    def attend(s):
        keys, values = kvbuf[s, 0], kvbuf[s, 1]
        length = meta[2 * c + s, pl.ds(1, 1), :]
        wide = jnp.concatenate([length] * (total // HD), axis=1)
        allowed = (query_at >= key_at) & (key_at < wide)
        for g in range(groups):
            query = rotated(acc[s, :, g * HD : (g + 1) * HD]).astype(jnp.bfloat16)
            scores = lax.dot_general(
                query, keys, (((1,), (1,)), ((), ())), preferred_element_type=jnp.float32
            ) * (1.0 / math.sqrt(HD))
            scores = jnp.where(allowed, scores, -jnp.inf)
            expo = jnp.exp(scores - jnp.max(scores, axis=1, keepdims=True))
            weights = (expo / jnp.sum(expo, axis=1, keepdims=True)).astype(jnp.bfloat16)
            att[s, x, :, g * HD : (g + 1) * HD] = jnp.dot(
                weights, values, preferred_element_type=jnp.float32
            ).astype(jnp.bfloat16)
        for direction in (0, 1):
            a_send(s, direction).start()

    def swapped(s):
        return remote(swap.at[s], kvall.at[2 * c + s], swap_s.at[s], swap_r.at[s], sibling)

    def d_copy(o):
        return remote(dests.at[z], dests.at[z], dest_s, dest_r, at_z(lax.rem(z + o, nz), c))

    def c1_copy(o):
        to = lax.rem(z + o, nz)
        return remote(
            kvall.at[:, pl.ds(pl.multiple_of(to * piece, piece), piece), :],
            spread.at[pl.ds(z * NX, NX)],
            c1_s, c1_r, at_z(to, c),
        )

    def send_dest(o, carry):
        d_copy(o).start()
        return carry

    def send_c1(o, carry):
        c1_copy(o).start()
        return carry

    lax.fori_loop(1, nz, send_dest, 0)
    for s in (0, 1):
        x_wait(s)
    project(q_cols, 2 * HD)
    for s in (0, 1):
        cache_rows(s)
        swapped(s).start()
    for k in range(half - LAG, half):
        o_step(k)
    def o_over(k, carry):
        o_partner(block_of(1, k), slot_of(1, k)).start()
        return carry

    lax.fori_loop(1, half, o_over, 0)

    for k in range(half - Y_LAG, half):
        for direction in (0, 1):
            partner_on(direction, k, slot_of(direction, k))
    partner_on(0, half, last)
    for s in (0, 1):
        swapped(s).wait_recv()
    lax.fori_loop(1, nz, send_c1, 0)
    spread[pl.ds(z * NX, NX)] = kvall[:, pl.ds(pl.multiple_of(z * piece, piece), piece), :]
    for which in (1, 2):
        w_all(0, q_cols // 2, (sib_s, sib_r.at[which])).wait_recv()
    project(0, q_cols)
    o_hop(0, far, last).wait_recv()
    o_sibling(far, last).start()
    o_partner(far, last).start()
    attend(0)
    attend(1)
    pass_attended(0)
    def d_all():
        blk = dests.at[pl.ds(0, nz - 1)]
        return remote(blk, blk, dest_s, dest_r, sibling)

    def c1_all():
        blk = spread.at[pl.ds(0, NX * (nz - 1))]
        return remote(blk, blk, c1_s, c1_r, sibling)

    d_all().wait_recv()
    c1_all().wait_recv()
    all_dests = dests[...].reshape(nz, HD)
    lanes = lax.broadcasted_iota(jnp.int32, (nz, HD), 1)
    prompt = lax.broadcasted_iota(jnp.int32, (nz, HD), 0) * NX
    source = jnp.zeros((nz, HD), jnp.int32)
    for j in range(NX):
        slot = jnp.sum(jnp.where(lanes == j, all_dests, 0), axis=1, keepdims=True)
        source += jnp.where(slot == lanes, prompt + j, 0)
    srcv[...] = jnp.minimum(jnp.sum(source, axis=0, keepdims=True), NX * nz - 1)
    to_scalars = pltpu.make_async_copy(srcv, srcs, src_l)
    to_scalars.start()
    to_scalars.wait()

    def reorder(d, carry):
        for j in range(NX):
            perm[j, d] = spread[srcs[0, j * nz + d]]
        return carry

    lax.fori_loop(0, nz, reorder, 0, unroll=4)

    def c2_copy(o):
        to = lax.rem(z + o, nz)
        return remote(perm.at[:, to], heads.at[:, z], c2_s, c2_r, at_z(to, c))

    def send_c2(o, carry):
        c2_copy(o).start()
        return carry

    lax.fori_loop(1, nz, send_c2, 0)
    heads[:, z] = perm[:, z]
    def o_all(semaphores):
        blk = wobuf.at[c, pl.ds(0, (nz - 1) * (QC // 2)), :]
        return remote(blk, blk, *semaphores, sibling)

    o_all((oy_s, oy_r)).wait_recv()

    def o_crossed(idx, carry):
        zs = jnp.where(
            idx == last, far,
            jnp.where(idx < half - 1, block_of(0, idx + 1), block_of(1, idx + 2 - half)),
        )
        o_y_sibling(zs, idx).start()
        return carry

    lax.fori_loop(0, last + 1, o_crossed, 0)

    pass_attended(1)
    o_all((osib_s, osib_r)).wait_recv()
    o_all((oysib_s, oysib_r)).wait_recv()
    o_own_sibling().wait_recv()

    def head_rows(s, xs):
        core = lax.div(xs, 2)
        cols = pl.ds(pl.multiple_of(lax.rem(xs, 2) * q_cols, q_cols), q_cols)
        return lax.dot_general(
            att[s, xs], wobuf[core, :, cols], (((1,), (1,)), ((), ())),
            preferred_element_type=jnp.float32,
        )

    for s in (0, 1):
        oacc[s] = head_rows(s, x)
        for direction in (0, 1):
            oacc[s] += head_rows(s, lax.rem(x + (NX - 1 if direction == 0 else 1), NX))

    width = oacc.shape[2]

    def out_cols(xs):
        return pl.ds(pl.multiple_of(lax.rem(xs, 2) * width, width), width)

    def out_copy(s):
        return remote(
            obuf.at[s], out_hbm.at[:, out_cols(x)], out_s.at[s, 0], out_r.at[lax.rem(x, 2)],
            (part, (2 * c + s) * nz + z, lax.div(x, 2)),
        )

    def out_here(s):
        return pltpu.make_async_copy(obuf.at[s], out_hbm.at[:, out_cols(x)], out_l)

    def out_rows(direction):
        return pl.ds(direction * (total // 2), total // 2)

    def out_first(s, direction):
        return remote(
            obuf.at[s, out_rows(direction)], relay.at[direction], out_s.at[s, direction],
            relay_r.at[direction], at_x(1 if direction == 0 else -1, c),
        )

    def out_second(direction):
        source = lax.rem(x + (NX - 1 if direction == 0 else 1), NX)
        return remote(
            relay.at[direction], out_hbm.at[out_rows(direction), out_cols(source)],
            relay_s.at[direction], out_r.at[lax.rem(source, 2)],
            at_x(1 if direction == 0 else -1, lax.div(source, 2)),
        )

    def relays(direction):
        to = lax.rem(x + (1 if direction == 0 else NX - 1), NX)
        return lax.div(to, 2) == c

    for s in (0, 1):
        for direction in (0, 1):
            a_forward(s, direction).wait_recv()
        obuf[s] = (oacc[s] + head_rows(s, lax.rem(x + 2, NX))).astype(jnp.bfloat16)

        @pl.when(away(s) == 2)
        def _(s=s):
            for direction in (0, 1):
                out_first(s, direction).start()

        pl.when((away(s) == 1) | (away(s) == 3))(lambda s=s: out_copy(s).start())
        pl.when(away(s) == 0)(lambda s=s: out_here(s).start())

    for direction in (0, 1):
        @pl.when(relays(direction))
        def _(direction=direction):
            out_first(0, direction).wait_recv()
            out_second(direction).start()

    def c2_all():
        blk = heads.at[:, pl.ds(0, nz - 1)]
        return remote(blk, blk, c2_s, c2_r, sibling)

    c2_all().wait_recv()

    def c3_copy(o, t):
        return remote(
            heads.at[lax.rem(x + o, NX), pl.ds(t * half, half)], kv_hbm.at[c, x, :, :, :],
            c3_s, c3_r, at_x(o, t),
        )

    def c3_here():
        return pltpu.make_async_copy(heads.at[x, pl.ds(c * half, half)], kv_hbm.at[c, x, :, :, :], c3_l)

    for o in range(1, NX):
        for t in (0, 1):
            c3_copy(o, t).start()
    c3_copy(0, 1 - c).start()
    c3_here().start()

    def c3_all():
        blk = heads.at[:, pl.ds(0, (2 * NX - 1) * half // NX)]
        return remote(blk, blk, c3_s, c3_r, sibling)

    c3_all().wait_recv()
    c3_here().wait()
    c3_all().wait_send()
    for i in (0, 1):
        @pl.when(2 * c + i != x)
        def _(i=i):
            cols = pl.ds(i * width, width)
            remote(obuf.at[0], out_hbm.at[:, cols], out_s.at[0, 0], out_r.at[i], sibling).wait_recv()

    for s in (0, 1):
        @pl.when(away(s) == 2)
        def _(s=s):
            for direction in (0, 1):
                out_first(s, direction).wait_send()

        pl.when((away(s) == 1) | (away(s) == 3))(lambda s=s: out_copy(s).wait_send())
        pl.when(away(s) == 0)(lambda s=s: out_here(s).wait())
        pl.when(relays(s))(lambda s=s: out_second(s).wait_send())
        for direction in (0, 1):
            a_send(s, direction).wait_send()
        for direction in (0, 1):
            a_forward(s, direction).wait_send()
    for b in (0, 1):
        @pl.when(2 * c + b != x)
        def _(b=b):
            for copy in w0(b):
                copy.wait_send()

    for o in range(1, NX):
        meta_copy(o).wait_send()

    @pl.when(is_source)
    def _():
        for i in range(4):
            for direction in (0, 1):
                x_send(direction, i).wait_send()

    for s in (0, 1):
        for i in (0, 1):
            pl.when(away(s) == 1)(lambda s=s, i=i: x_forward(s, i, 0).wait_send())
            pl.when(away(s) == 3)(lambda s=s, i=i: x_forward(s, 2 + i, 1).wait_send())
        swapped(s).wait_send()
    own_to_sibling().wait_send()
    o_own_sibling().wait_send()

    for sent in (d_all(), c1_all(), c2_all()):
        sent.wait_send()
    w_all(0, q_cols, (ring_s, ring_r.at[0, 0])).wait_send()
    w_all(0, columns, (sib_s, sib_r.at[0])).wait_send()
    w_all(0, q_cols // 2, (y_s, y_r.at[0])).wait_send()
    for pair in ((o_s, o_r.at[0]), (osib_s, osib_r), (oy_s, oy_r), (oysib_s, oysib_r)):
        o_all(pair).wait_send()


def on_device(normed, q_weight, kv_weight, o_weight, lengths, destinations):
    tokens = normed[0]
    total, width = tokens.shape
    nz = lax.axis_size("dp") // NX
    rows = q_weight.shape[0]
    q_cols = q_weight.shape[1] // 2
    kv_rows = kv_weight.reshape(rows, -1)
    o_t = o_weight.T
    cosine, sine = tables(total)
    columns = q_cols + 2 * HD
    o_cols = rows * nz
    piece = total // nz
    hops = nz - 1
    bf16, f32 = jnp.bfloat16, jnp.float32
    dma = pltpu.SemaphoreType.DMA
    scratch = [
        pltpu.VMEM((NX, width // NX, columns), bf16),
        pltpu.VMEM((2, o_cols, o_weight.shape[0]), bf16),
        pltpu.VMEM((2, total, width), bf16),
        pltpu.VMEM((2, NX, total, q_cols), bf16),
        pltpu.VMEM((2, total, columns), f32),
        pltpu.VMEM((2, total, o_cols), f32),
        pltpu.VMEM((2, total, o_cols), bf16),
        pltpu.VMEM((NX, 2, HD), jnp.int32),
        pltpu.VMEM((nz, 1, HD), jnp.int32),
        pltpu.VMEM((1, HD), jnp.int32),
        pltpu.SMEM((1, HD), jnp.int32),
        pltpu.VMEM((NX, total, HD), bf16),
        pltpu.VMEM((2, total, HD), bf16),
        pltpu.VMEM((NX * nz, piece, HD), bf16),
        pltpu.VMEM((NX, nz, piece, HD), bf16),
        pltpu.VMEM((NX, nz, piece, HD), bf16),
    ]
    shapes = [
        (NX,), (NX,), (2, 3), (2,), None, (hops, 2), None, (3,), None, (hops,), None, None,
        None, (hops,), None, None, None, None, None, (2, 4), (2, 2), (2, 4), (2, 2), (2, 2), (2, 4), (2,), (2,),
        None, None, None, None, None, None, None, None, None, None, (2, 2), (2,), None,
    ]
    scratch += [dma if shape is None else dma(shape) for shape in shapes]
    scratch.append(pltpu.SemaphoreType.REGULAR((2,)))
    scratch += [pltpu.VMEM((2, 2, total, HD), bf16), pltpu.VMEM((2, total // 2, o_cols), bf16), dma((2,)), dma((2,))]
    scratch += [dma] * 4
    scratch += [pltpu.VMEM(a.shape, a.dtype) for a in (q_weight, kv_rows, o_t, cosine, sine)] + [dma((5,))]
    smem = pl.BlockSpec(memory_space=pltpu.SMEM)
    vmem = pl.BlockSpec(memory_space=pltpu.VMEM)
    any_space = pl.BlockSpec(memory_space=pl.ANY)
    projected, cache = pl.pallas_call(
        functools.partial(kernel, nz),
        out_shape=(
            pltpu.VMEM((total, 2 * o_cols), bf16),
            pltpu.VMEM((2, NX, nz // 2, piece, HD), bf16),
        ),
        in_specs=[any_space] * 6 + [smem, smem],
        out_specs=(vmem, vmem),
        scratch_shapes=scratch,
        compiler_params=pltpu.CompilerParams(
            collective_id=0, has_side_effects=True, vmem_limit_bytes=60 * 1024 * 1024
        ),
    )(tokens, q_weight, kv_rows, o_t, cosine, sine, destinations, lengths)
    return (projected[None], cache.reshape(1, 2, NX, total // 2, HD))


def solution(mesh):
    placed = (
        P(("parts", "dp"), None, None),
        P("dp", "tensor"),
        P("dp", None, "tensor"),
        P("tensor", "dp"),
        P(("parts", "dp")),
        P(("parts", "dp")),
    )
    return jax.shard_map(
        on_device,
        mesh=mesh,
        in_specs=placed,
        out_specs=(
            P(("parts", "dp"), None, "tensor"),
            P(("parts", "dp"), None, None, "tensor", None),
        ),
        check_vma=False,
    )
```

```python
import functools
import math

import jax
import jax.numpy as jnp
import numpy as np
from jax import lax
from jax.experimental import pallas as pl
from jax.experimental.pallas import tpu as pltpu
from jax.sharding import PartitionSpec as P

HD = 128
ROPE_BASE = 500000.0
NX = 4
KC = 1024
QC = 64
LAG = 1
Y_LAG = 3


def tables(total):
    half = HD // 2
    steps = np.arange(half, dtype=np.float32) * np.float32(2.0 / HD)
    freq = np.power(np.float32(ROPE_BASE), -steps)
    angle = np.arange(total, dtype=np.float32)[:, None] * freq[None, :]
    cosine, sine = np.cos(angle), np.sin(angle)
    return (
        jnp.asarray(np.concatenate([cosine, cosine], axis=-1)),
        jnp.asarray(np.concatenate([-sine, sine], axis=-1)),
    )


def remote(src, dst, send, recv, device):
    return pltpu.make_async_remote_copy(
        src_ref=src,
        dst_ref=dst,
        send_sem=send,
        recv_sem=recv,
        device_id=device,
        device_id_type=pl.DeviceIdType.MESH,
    )


def kernel(
    nz, x_hbm, q_hbm, kv_hbm_in, o_hbm, cos_hbm, sin_hbm, dest_ref, length_ref, out_hbm, kv_hbm,
    wbuf, wobuf, xbuf, att, acc, oacc, obuf, meta, dests, srcv, srcs, kvall, swap, spread, perm, heads,
    meta_s, meta_r, w0_s, w0_r, ring_s, ring_r, sib_s, sib_r, y_s, y_r, own_s, own_r,
    o_s, o_r, osib_s, osib_r, oown_s, oown_r, x_l, x_s, xf_s, x_r, a_s, af_s, a_r, swap_s, swap_r,
    dest_s, dest_r, c1_s, c1_r, src_l, c2_s, c2_r, c3_s, c3_r, c3_l, out_s, out_r, out_l, ready, kvbuf, relay, relay_s, relay_r,
    oy_s, oy_r, oysib_s, oysib_r, q_ref, kv_pair, kv_ref, o_t, cos_ref, sin_ref, load,
):
    part, dp, c = lax.axis_index("parts"), lax.axis_index("dp"), lax.axis_index("tensor")
    x, z = lax.div(dp, nz), lax.rem(dp, nz)
    half = nz // 2
    yb = lax.rem(part, 2)
    mate = part + 1 - 2 * yb
    rows = q_ref.shape[0]
    total = xbuf.shape[1]
    piece = total // nz
    last = 2 * (half - 1)

    def at_x(offset, core):
        return (part, lax.rem(x + offset + NX, NX) * nz + z, core)

    def at_z(where, core):
        return (part, x * nz + where, core)

    sibling = (part, dp, 1 - c)
    partner = (mate, dp, c)
    up, down = lax.rem(z + 1, nz), lax.rem(z + nz - 1, nz)

    loads = [
        pltpu.make_async_copy(src, dst, load.at[i])
        for i, (src, dst) in enumerate(
            ((kv_hbm_in, kv_pair), (q_hbm, q_ref), (o_hbm, o_t), (cos_hbm, cos_ref), (sin_hbm, sin_ref))
        )
    ]
    for copy in loads:
        copy.start()

    barrier = pltpu.get_barrier_semaphore()

    def greet(semaphore, device):
        pl.semaphore_signal(semaphore, inc=1, device_id=device, device_id_type=pl.DeviceIdType.MESH)

    greeted = [at_x(o, k) for o in range(1, NX) for k in (0, 1)] + [sibling, partner]
    for device in greeted:
        greet(barrier, device)
    pl.when(z != 0)(lambda: greet(barrier, at_z(up, c)))
    pl.when(z == 1)(lambda: greet(barrier, at_z(down, c)))
    loads[0].wait()
    pair = kv_pair[...].astype(jnp.float32)
    for i in (0, 1):
        kv_ref[:, 2 * HD * i : 2 * HD * (i + 1)] = pair[:, i, :].astype(jnp.bfloat16)
    pl.semaphore_wait(
        barrier, len(greeted) + jnp.where(z == 1, 0, 1) + jnp.where(z == 0, 1, 0)
    )
    pl.when(z != 1)(lambda: greet(ready.at[0], at_z(down, c)))
    for copy in loads[1:]:
        copy.wait()
    pl.when(z == 0)(lambda: greet(ready.at[1], at_z(up, c)))

    columns = wbuf.shape[2]
    q_cols = columns - 2 * HD

    def w_block(xs, zs):
        return wbuf.at[xs, pl.ds(pl.multiple_of(zs * rows, rows), rows), :]

    def w0_parts(b):
        return (
            (q_ref, b * q_cols, 0, q_cols),
            (kv_ref, b * HD, q_cols, HD),
            (kv_ref, (2 + b) * HD, q_cols + HD, HD),
        )

    def w0(b):
        block = w_block(x, z)
        return [
            remote(
                src.at[:, pl.ds(start, size)], block.at[:, pl.ds(to, size)], w0_s.at[b, i],
                w0_r.at[lax.rem(x, 2)], (part, (2 * c + b) * nz + z, lax.div(x, 2)),
            )
            for i, (src, start, to, size) in enumerate(w0_parts(b))
        ]

    for b in (0, 1):
        @pl.when(2 * c + b != x)
        def _(b=b):
            for copy in w0(b):
                copy.start()

    for b in (0, 1):
        @pl.when(2 * c + b == x)
        def _(b=b):
            block = w_block(x, z)
            for src, start, to, size in w0_parts(b):
                block[:, to : to + size] = src[:, start : start + size]

    meta[x] = jnp.concatenate(
        [jnp.full((1, HD), dest_ref[0], jnp.int32), jnp.full((1, HD), length_ref[0], jnp.int32)]
    )

    def meta_copy(o):
        return remote(meta.at[x], meta.at[x], meta_s.at[o], meta_r.at[o], at_x(o, c))

    for o in range(1, NX):
        meta_copy(o).start()

    quarter = total // 4

    def away(s):
        return lax.rem(x - 2 * c - s + 2 * NX, NX)

    is_source = lax.div(x, 2) == c
    mine = lax.rem(x, 2)

    def x_rows(q):
        return pl.ds(q * quarter, quarter)

    def x_send(direction, q):
        return remote(
            x_hbm.at[x_rows(q)], xbuf.at[mine, x_rows(q)], x_s.at[direction, q], x_r.at[mine, q],
            at_x(1 if direction == 0 else -1, c),
        )

    def x_local():
        return pltpu.make_async_copy(x_hbm, xbuf.at[mine], x_l)

    def x_forward(s, q, direction):
        return remote(
            xbuf.at[s, x_rows(q)], xbuf.at[s, x_rows(q)], xf_s.at[s, q % 2], x_r.at[s, q],
            at_x(1 if direction == 0 else -1, c),
        )

    @pl.when(is_source)
    def _():
        for i in range(4):
            x_send(0, i).start()
            x_send(1, (i + 2) % 4).start()
        x_local().start()

    def x_arrival(s, q):
        rows_of = xbuf.at[s, x_rows(q)]
        return remote(rows_of, rows_of, xf_s.at[s, q % 2], x_r.at[s, q], sibling)

    def pass_on(i):
        for s in (0, 1):
            @pl.when(away(s) == 1)
            def _(s=s):
                x_forward(s, i, 0).wait_recv()
                x_forward(s, i, 0).start()

            @pl.when(away(s) == 3)
            def _(s=s):
                x_forward(s, 2 + i, 1).wait_recv()
                x_forward(s, 2 + i, 1).start()

    def w_part(zs, core, which):
        cols = pl.ds(q_cols, 2 * HD)
        if which:
            at = yb if which == 1 else 1 - yb
            cols = pl.ds(pl.multiple_of(at * (q_cols // 2), q_cols // 2), q_cols // 2)
        return wbuf.at[pl.ds(2 * core, 2), pl.ds(pl.multiple_of(zs * rows, rows), rows), cols]

    def hop(direction, zs, idx, which):
        blk = w_part(zs, c, which)
        return remote(
            blk, blk, ring_s, ring_r.at[idx, which],
            at_z(up if direction == 0 else down, c),
        )

    def to_sibling(zs, idx, which):
        blk = w_part(zs, c, which)
        return remote(blk, blk, sib_s, sib_r.at[which], sibling)

    def to_partner(zs, idx):
        blk = w_part(zs, c, 1)
        return remote(blk, blk, y_s, y_r.at[idx], partner)

    def from_partner(zs, idx):
        blk = w_part(zs, c, 2)
        return remote(blk, blk, y_s, y_r.at[idx], partner)

    def own_to_sibling():
        blk = wbuf.at[pl.ds(2 * c, 2), pl.ds(pl.multiple_of(z * rows, rows), rows), :]
        return remote(blk, blk, own_s, own_r, sibling)

    def o_block(zs, core):
        return wobuf.at[core, pl.ds(pl.multiple_of(zs * QC, QC), QC), :]

    def o_part(zs, which):
        start = pl.multiple_of(zs * QC + which * (QC // 2), QC // 2)
        return wobuf.at[c, pl.ds(start, QC // 2), :]

    def o_hop(direction, zs, idx, src=None):
        blk = o_part(zs, yb)
        return remote(
            blk if src is None else src, blk, o_s, o_r.at[idx],
            at_z(up if direction == 0 else down, c),
        )

    def o_sibling(zs, idx):
        blk = o_part(zs, yb)
        return remote(blk, blk, osib_s, osib_r, sibling)

    def o_partner(zs, idx):
        blk = o_part(zs, yb)
        return remote(blk, blk, oy_s, oy_r, partner)

    def o_y_sibling(zs, idx):
        blk = o_part(zs, 1 - yb)
        return remote(blk, blk, oysib_s, oysib_r, sibling)

    def o_own_sibling():
        return remote(o_t, o_block(z, c), oown_s, oown_r, sibling)

    for i in (0, 1):
        @pl.when(2 * c + i != x)
        def _(i=i):
            blk = w_block(2 * c + i, z)
            remote(blk, blk, w0_s.at[0, 0], w0_r.at[i], sibling).wait_recv()

    first = (0, half - 1)
    own_to_sibling().start()
    pl.when(z != 0)(lambda: pl.semaphore_wait(ready.at[0], 1))
    for h in (0, 1):
        hop(0, z, first[0], h).start()
    pl.when(z == 1)(lambda: pl.semaphore_wait(ready.at[1], 1))
    for h in (0, 1):
        hop(1, z, first[1], h).start()
    o_block(z, c)[...] = o_t[...]

    def block_of(direction, k):
        return lax.rem(z + (nz - k if direction == 0 else k), nz)

    def slot_of(direction, k):
        return direction * (half - 1) + k - 1

    def partner_on(direction, k, idx):
        zs = block_of(direction, k)
        from_partner(zs, idx).wait_recv()
        to_sibling(zs, idx, 2).start()

    def w_half(direction, k, h):
        idx = slot_of(direction, k)
        zs = block_of(direction, k)
        hop(direction, zs, idx, h).wait_recv()

        @pl.when((k < half - 1) | (c == direction))
        def _():
            hop(direction, zs, jnp.where(k == half - 1, last, idx + 1), h).start()

    def w_rest(direction, k):
        idx = slot_of(direction, k)
        zs = block_of(direction, k)
        to_sibling(zs, idx, 0).start()
        to_sibling(zs, idx, 1).start()
        to_partner(zs, idx).start()

    def o_step(k):
        for direction in (0, 1):
            idx = slot_of(direction, k)
            zs = block_of(direction, k)
            o_hop(direction, zs, idx).wait_recv()

            @pl.when((k < half - 1) | (c == direction))
            def _(direction=direction, idx=idx, zs=zs):
                o_hop(direction, zs, jnp.where(k == half - 1, last, idx + 1)).start()

            o_sibling(zs, idx).start()
            if direction == 0:
                o_partner(zs, idx).start()

    def ring_step(k, carry):
        for h in (0, 1):
            for direction in (0, 1):
                w_half(direction, k, h)
        for direction in (0, 1):
            w_rest(direction, k)
        @pl.when(k > LAG)
        def _():
            o_step(k - LAG)

        @pl.when(k > Y_LAG)
        def _():
            for direction in (0, 1):
                partner_on(direction, k - Y_LAG, slot_of(direction, k - Y_LAG))

        return carry

    for direction in (0, 1):
        o_hop(direction, z, first[direction], o_t.at[pl.ds(pl.multiple_of(yb * (QC // 2), QC // 2), QC // 2)]).start()
    o_own_sibling().start()
    lax.fori_loop(1, 3, ring_step, 0)
    pass_on(0)
    lax.fori_loop(3, 5, ring_step, 0)
    pass_on(1)
    lax.fori_loop(5, half, ring_step, 0)
    far = block_of(0, half)
    for which in (0, 1):
        hop(0, far, last, which).wait_recv()
        to_sibling(far, last, which).start()
    to_partner(far, last).start()

    def w_all(start, size, semaphores):
        blk = wbuf.at[pl.ds(0, 2), pl.ds(0, (nz - 1) * rows), pl.ds(start, size)]
        return remote(blk, blk, *semaphores, sibling)

    w_all(q_cols, 2 * HD, (sib_s, sib_r.at[0])).wait_recv()
    own_to_sibling().wait_recv()
    for o in range(1, NX):
        meta_copy(o).wait_recv()

    lane = lax.broadcasted_iota(jnp.int32, (1, HD), 1)
    row = jnp.zeros((1, HD), jnp.int32)
    for j in range(NX):
        row = jnp.where(lane == j, meta[j, pl.ds(0, 1), :], row)
    dests[z] = row

    cosine, sine = cos_ref[...], sin_ref[...]

    def rotated(u):
        return u * cosine + pltpu.roll(u, HD // 2, 1) * sine

    groups = q_cols // HD
    key_at = lax.broadcasted_iota(jnp.int32, (total, total), 1)
    query_at = lax.broadcasted_iota(jnp.int32, (total, total), 0)
    position = lax.broadcasted_iota(jnp.int32, (total, HD), 0)

    def a_send(s, direction):
        return remote(
            att.at[s, x], att.at[s, x], a_s.at[s, direction], a_r.at[s, direction],
            at_x(1 if direction == 0 else -1, c),
        )

    def a_forward(s, direction):
        source = lax.rem(x + (NX - 1 if direction == 0 else 1), NX)
        blk = att.at[s, source, pl.ds(direction * (total // 2), total // 2)]
        return remote(
            blk, blk, af_s.at[s, direction], a_r.at[s, 2 + direction],
            at_x(1 if direction == 0 else -1, c),
        )

    def pass_attended(s):
        for direction in (0, 1):
            a_send(s, direction).wait_recv()
        for direction in (0, 1):
            a_forward(s, direction).start()

    def x_wait(s):
        @pl.when(away(s) == 0)
        def _():
            x_local().wait()

        @pl.when((away(s) == 1) | (away(s) == 2))
        def _():
            for q in (2, 3):
                x_arrival(s, q).wait_recv()

        @pl.when((away(s) == 3) | (away(s) == 2))
        def _():
            for q in (0, 1):
                x_arrival(s, q).wait_recv()

    def project(start, size):
        cols = pl.ds(start, size)
        per = nz * rows // KC

        def part_of(i):
            deep = pl.ds(pl.multiple_of(i * KC, KC), KC)
            inside = pl.ds(pl.multiple_of(lax.rem(i, per) * KC, KC), KC)
            both = xbuf[:, :, deep].reshape(2 * total, KC)
            return jnp.dot(
                both, wbuf[lax.div(i, per), inside, cols], preferred_element_type=jnp.float32
            ).reshape(2, total, size)

        acc[:, :, cols] = part_of(0)

        def add(i, carry):
            acc[:, :, cols] += part_of(i)
            return carry

        lax.fori_loop(1, xbuf.shape[2] // KC, add, 0)

    def cache_rows(s):
        length = meta[2 * c + s, pl.ds(1, 1), :]
        keys = rotated(acc[s, :, q_cols : q_cols + HD])
        values = acc[s, :, q_cols + HD :]
        live = position < length
        kept_keys = jnp.where(live, keys, 0.0).astype(jnp.bfloat16)
        kept_values = jnp.where(live, values, 0.0).astype(jnp.bfloat16)

        @pl.when(c == 0)
        def _():
            kvall[s] = kept_keys
            swap[s] = kept_values

        @pl.when(c == 1)
        def _():
            kvall[2 + s] = kept_values
            swap[s] = kept_keys

        kvbuf[s, 0] = keys.astype(jnp.bfloat16)
        kvbuf[s, 1] = values.astype(jnp.bfloat16)

    def attend(s):
        keys, values = kvbuf[s, 0], kvbuf[s, 1]
        length = meta[2 * c + s, pl.ds(1, 1), :]
        wide = jnp.concatenate([length] * (total // HD), axis=1)
        allowed = (query_at >= key_at) & (key_at < wide)
        for g in range(groups):
            query = rotated(acc[s, :, g * HD : (g + 1) * HD]).astype(jnp.bfloat16)
            scores = lax.dot_general(
                query, keys, (((1,), (1,)), ((), ())), preferred_element_type=jnp.float32
            ) * (1.0 / math.sqrt(HD))
            scores = jnp.where(allowed, scores, -jnp.inf)
            expo = jnp.exp(scores - jnp.max(scores, axis=1, keepdims=True))
            weights = (expo / jnp.sum(expo, axis=1, keepdims=True)).astype(jnp.bfloat16)
            att[s, x, :, g * HD : (g + 1) * HD] = jnp.dot(
                weights, values, preferred_element_type=jnp.float32
            ).astype(jnp.bfloat16)
        for direction in (0, 1):
            a_send(s, direction).start()

    def swapped(s):
        return remote(swap.at[s], kvall.at[2 * c + s], swap_s.at[s], swap_r.at[s], sibling)

    def d_copy(o):
        return remote(dests.at[z], dests.at[z], dest_s, dest_r, at_z(lax.rem(z + o, nz), c))

    def c1_copy(o):
        to = lax.rem(z + o, nz)
        return remote(
            kvall.at[:, pl.ds(pl.multiple_of(to * piece, piece), piece), :],
            spread.at[pl.ds(z * NX, NX)],
            c1_s, c1_r, at_z(to, c),
        )

    def send_dest(o, carry):
        d_copy(o).start()
        return carry

    def send_c1(o, carry):
        c1_copy(o).start()
        return carry

    for s in (0, 1):
        x_wait(s)
    project(q_cols, 2 * HD)
    for s in (0, 1):
        cache_rows(s)
        swapped(s).start()
    for k in range(half - LAG, half):
        o_step(k)
    def o_over(k, carry):
        o_partner(block_of(1, k), slot_of(1, k)).start()
        return carry

    lax.fori_loop(1, half, o_over, 0)

    for k in range(half - Y_LAG, half):
        for direction in (0, 1):
            partner_on(direction, k, slot_of(direction, k))
    partner_on(0, half, last)
    for s in (0, 1):
        swapped(s).wait_recv()
    lax.fori_loop(1, nz, send_c1, 0)
    spread[pl.ds(z * NX, NX)] = kvall[:, pl.ds(pl.multiple_of(z * piece, piece), piece), :]
    for which in (1, 2):
        w_all(0, q_cols // 2, (sib_s, sib_r.at[which])).wait_recv()
    project(0, q_cols)
    lax.fori_loop(1, nz, send_dest, 0)
    o_hop(0, far, last).wait_recv()
    o_sibling(far, last).start()
    o_partner(far, last).start()
    attend(0)
    attend(1)
    pass_attended(0)
    def d_all():
        blk = dests.at[pl.ds(0, nz - 1)]
        return remote(blk, blk, dest_s, dest_r, sibling)

    def c1_all():
        blk = spread.at[pl.ds(0, NX * (nz - 1))]
        return remote(blk, blk, c1_s, c1_r, sibling)

    d_all().wait_recv()
    c1_all().wait_recv()
    all_dests = dests[...].reshape(nz, HD)
    lanes = lax.broadcasted_iota(jnp.int32, (nz, HD), 1)
    prompt = lax.broadcasted_iota(jnp.int32, (nz, HD), 0) * NX
    source = jnp.zeros((nz, HD), jnp.int32)
    for j in range(NX):
        slot = jnp.sum(jnp.where(lanes == j, all_dests, 0), axis=1, keepdims=True)
        source += jnp.where(slot == lanes, prompt + j, 0)
    srcv[...] = jnp.minimum(jnp.sum(source, axis=0, keepdims=True), NX * nz - 1)
    to_scalars = pltpu.make_async_copy(srcv, srcs, src_l)
    to_scalars.start()
    to_scalars.wait()

    def reorder(d, carry):
        for j in range(NX):
            perm[j, d] = spread[srcs[0, j * nz + d]]
        return carry

    lax.fori_loop(0, nz, reorder, 0, unroll=4)

    def c2_copy(o):
        to = lax.rem(z + o, nz)
        return remote(perm.at[:, to], heads.at[:, z], c2_s, c2_r, at_z(to, c))

    def send_c2(o, carry):
        c2_copy(o).start()
        return carry

    lax.fori_loop(1, nz, send_c2, 0)
    heads[:, z] = perm[:, z]
    def o_all(semaphores):
        blk = wobuf.at[c, pl.ds(0, (nz - 1) * (QC // 2)), :]
        return remote(blk, blk, *semaphores, sibling)

    o_all((oy_s, oy_r)).wait_recv()

    def o_crossed(idx, carry):
        zs = jnp.where(
            idx == last, far,
            jnp.where(idx < half - 1, block_of(0, idx + 1), block_of(1, idx + 2 - half)),
        )
        o_y_sibling(zs, idx).start()
        return carry

    lax.fori_loop(0, last + 1, o_crossed, 0)

    pass_attended(1)
    o_all((osib_s, osib_r)).wait_recv()
    o_all((oysib_s, oysib_r)).wait_recv()
    o_own_sibling().wait_recv()

    def head_rows(s, xs):
        core = lax.div(xs, 2)
        cols = pl.ds(pl.multiple_of(lax.rem(xs, 2) * q_cols, q_cols), q_cols)
        return lax.dot_general(
            att[s, xs], wobuf[core, :, cols], (((1,), (1,)), ((), ())),
            preferred_element_type=jnp.float32,
        )

    for s in (0, 1):
        oacc[s] = head_rows(s, x)
        for direction in (0, 1):
            oacc[s] += head_rows(s, lax.rem(x + (NX - 1 if direction == 0 else 1), NX))

    width = oacc.shape[2]

    def out_cols(xs):
        return pl.ds(pl.multiple_of(lax.rem(xs, 2) * width, width), width)

    def out_copy(s):
        return remote(
            obuf.at[s], out_hbm.at[:, out_cols(x)], out_s.at[s, 0], out_r.at[lax.rem(x, 2)],
            (part, (2 * c + s) * nz + z, lax.div(x, 2)),
        )

    def out_here(s):
        return pltpu.make_async_copy(obuf.at[s], out_hbm.at[:, out_cols(x)], out_l)

    def out_rows(direction):
        return pl.ds(direction * (total // 2), total // 2)

    def out_first(s, direction):
        return remote(
            obuf.at[s, out_rows(direction)], relay.at[direction], out_s.at[s, direction],
            relay_r.at[direction], at_x(1 if direction == 0 else -1, c),
        )

    def out_second(direction):
        source = lax.rem(x + (NX - 1 if direction == 0 else 1), NX)
        return remote(
            relay.at[direction], out_hbm.at[out_rows(direction), out_cols(source)],
            relay_s.at[direction], out_r.at[lax.rem(source, 2)],
            at_x(1 if direction == 0 else -1, lax.div(source, 2)),
        )

    def relays(direction):
        to = lax.rem(x + (1 if direction == 0 else NX - 1), NX)
        return lax.div(to, 2) == c

    for s in (0, 1):
        for direction in (0, 1):
            a_forward(s, direction).wait_recv()
        obuf[s] = (oacc[s] + head_rows(s, lax.rem(x + 2, NX))).astype(jnp.bfloat16)

        @pl.when(away(s) == 2)
        def _(s=s):
            for direction in (0, 1):
                out_first(s, direction).start()

        pl.when((away(s) == 1) | (away(s) == 3))(lambda s=s: out_copy(s).start())
        pl.when(away(s) == 0)(lambda s=s: out_here(s).start())

    for direction in (0, 1):
        @pl.when(relays(direction))
        def _(direction=direction):
            out_first(0, direction).wait_recv()
            out_second(direction).start()

    def c2_all():
        blk = heads.at[:, pl.ds(0, nz - 1)]
        return remote(blk, blk, c2_s, c2_r, sibling)

    c2_all().wait_recv()

    def c3_copy(o, t):
        return remote(
            heads.at[lax.rem(x + o, NX), pl.ds(t * half, half)], kv_hbm.at[c, x, :, :, :],
            c3_s, c3_r, at_x(o, t),
        )

    def c3_here():
        return pltpu.make_async_copy(heads.at[x, pl.ds(c * half, half)], kv_hbm.at[c, x, :, :, :], c3_l)

    for o in range(1, NX):
        for t in (0, 1):
            c3_copy(o, t).start()
    c3_copy(0, 1 - c).start()
    c3_here().start()

    def c3_all():
        blk = heads.at[:, pl.ds(0, (2 * NX - 1) * half // NX)]
        return remote(blk, blk, c3_s, c3_r, sibling)

    c3_all().wait_recv()
    c3_here().wait()
    c3_all().wait_send()
    for i in (0, 1):
        @pl.when(2 * c + i != x)
        def _(i=i):
            cols = pl.ds(i * width, width)
            remote(obuf.at[0], out_hbm.at[:, cols], out_s.at[0, 0], out_r.at[i], sibling).wait_recv()

    for s in (0, 1):
        @pl.when(away(s) == 2)
        def _(s=s):
            for direction in (0, 1):
                out_first(s, direction).wait_send()

        pl.when((away(s) == 1) | (away(s) == 3))(lambda s=s: out_copy(s).wait_send())
        pl.when(away(s) == 0)(lambda s=s: out_here(s).wait())
        pl.when(relays(s))(lambda s=s: out_second(s).wait_send())
        for direction in (0, 1):
            a_send(s, direction).wait_send()
        for direction in (0, 1):
            a_forward(s, direction).wait_send()
    for b in (0, 1):
        @pl.when(2 * c + b != x)
        def _(b=b):
            for copy in w0(b):
                copy.wait_send()

    for o in range(1, NX):
        meta_copy(o).wait_send()

    @pl.when(is_source)
    def _():
        for i in range(4):
            for direction in (0, 1):
                x_send(direction, i).wait_send()

    for s in (0, 1):
        for i in (0, 1):
            pl.when(away(s) == 1)(lambda s=s, i=i: x_forward(s, i, 0).wait_send())
            pl.when(away(s) == 3)(lambda s=s, i=i: x_forward(s, 2 + i, 1).wait_send())
        swapped(s).wait_send()
    own_to_sibling().wait_send()
    o_own_sibling().wait_send()

    for sent in (d_all(), c1_all(), c2_all()):
        sent.wait_send()
    w_all(0, q_cols, (ring_s, ring_r.at[0, 0])).wait_send()
    w_all(0, columns, (sib_s, sib_r.at[0])).wait_send()
    w_all(0, q_cols // 2, (y_s, y_r.at[0])).wait_send()
    for pair in ((o_s, o_r.at[0]), (osib_s, osib_r), (oy_s, oy_r), (oysib_s, oysib_r)):
        o_all(pair).wait_send()


def on_device(normed, q_weight, kv_weight, o_weight, lengths, destinations):
    tokens = normed[0]
    total, width = tokens.shape
    nz = lax.axis_size("dp") // NX
    rows = q_weight.shape[0]
    q_cols = q_weight.shape[1] // 2
    o_t = o_weight.T
    cosine, sine = tables(total)
    columns = q_cols + 2 * HD
    o_cols = rows * nz
    piece = total // nz
    hops = nz - 1
    bf16, f32 = jnp.bfloat16, jnp.float32
    dma = pltpu.SemaphoreType.DMA
    scratch = [
        pltpu.VMEM((NX, width // NX, columns), bf16),
        pltpu.VMEM((2, o_cols, o_weight.shape[0]), bf16),
        pltpu.VMEM((2, total, width), bf16),
        pltpu.VMEM((2, NX, total, q_cols), bf16),
        pltpu.VMEM((2, total, columns), f32),
        pltpu.VMEM((2, total, o_cols), f32),
        pltpu.VMEM((2, total, o_cols), bf16),
        pltpu.VMEM((NX, 2, HD), jnp.int32),
        pltpu.VMEM((nz, 1, HD), jnp.int32),
        pltpu.VMEM((1, HD), jnp.int32),
        pltpu.SMEM((1, HD), jnp.int32),
        pltpu.VMEM((NX, total, HD), bf16),
        pltpu.VMEM((2, total, HD), bf16),
        pltpu.VMEM((NX * nz, piece, HD), bf16),
        pltpu.VMEM((NX, nz, piece, HD), bf16),
        pltpu.VMEM((NX, nz, piece, HD), bf16),
    ]
    shapes = [
        (NX,), (NX,), (2, 3), (2,), None, (hops, 2), None, (3,), None, (hops,), None, None,
        None, (hops,), None, None, None, None, None, (2, 4), (2, 2), (2, 4), (2, 2), (2, 2), (2, 4), (2,), (2,),
        None, None, None, None, None, None, None, None, None, None, (2, 2), (2,), None,
    ]
    scratch += [dma if shape is None else dma(shape) for shape in shapes]
    scratch.append(pltpu.SemaphoreType.REGULAR((2,)))
    scratch += [pltpu.VMEM((2, 2, total, HD), bf16), pltpu.VMEM((2, total // 2, o_cols), bf16), dma((2,)), dma((2,))]
    scratch += [dma] * 4
    scratch += [pltpu.VMEM(a.shape, a.dtype) for a in (q_weight, kv_weight, kv_weight.reshape(rows, -1), o_t, cosine, sine)]
    scratch.append(dma((5,)))
    smem = pl.BlockSpec(memory_space=pltpu.SMEM)
    vmem = pl.BlockSpec(memory_space=pltpu.VMEM)
    any_space = pl.BlockSpec(memory_space=pl.ANY)
    projected, cache = pl.pallas_call(
        functools.partial(kernel, nz),
        out_shape=(
            pltpu.VMEM((total, 2 * o_cols), bf16),
            pltpu.VMEM((2, NX, nz // 2, piece, HD), bf16),
        ),
        in_specs=[any_space] * 6 + [smem, smem],
        out_specs=(vmem, vmem),
        scratch_shapes=scratch,
        compiler_params=pltpu.CompilerParams(
            collective_id=0, has_side_effects=True, vmem_limit_bytes=60 * 1024 * 1024
        ),
    )(tokens, q_weight, kv_weight, o_t, cosine, sine, destinations, lengths)
    return (projected[None], cache.reshape(1, 2, NX, total // 2, HD))


def solution(mesh):
    placed = (
        P(("parts", "dp"), None, None),
        P("dp", "tensor"),
        P("dp", None, "tensor"),
        P("tensor", "dp"),
        P(("parts", "dp")),
        P(("parts", "dp")),
    )
    return jax.shard_map(
        on_device,
        mesh=mesh,
        in_specs=placed,
        out_specs=(
            P(("parts", "dp"), None, "tensor"),
            P(("parts", "dp"), None, None, "tensor", None),
        ),
        check_vma=False,
    )
```

```python
import functools
import math

import jax
import jax.numpy as jnp
import numpy as np
from jax import lax
from jax.experimental import pallas as pl
from jax.experimental.pallas import tpu as pltpu
from jax.sharding import PartitionSpec as P

HD = 128
ROPE_BASE = 500000.0
NX = 4
KC = 1024
QC = 64
LAG = 1
Y_LAG = 3


def tables(total):
    half = HD // 2
    steps = np.arange(half, dtype=np.float32) * np.float32(2.0 / HD)
    freq = np.power(np.float32(ROPE_BASE), -steps)
    angle = np.arange(total, dtype=np.float32)[:, None] * freq[None, :]
    cosine, sine = np.cos(angle), np.sin(angle)
    return (
        jnp.asarray(np.concatenate([cosine, cosine], axis=-1)),
        jnp.asarray(np.concatenate([-sine, sine], axis=-1)),
    )


def remote(src, dst, send, recv, device):
    return pltpu.make_async_remote_copy(
        src_ref=src,
        dst_ref=dst,
        send_sem=send,
        recv_sem=recv,
        device_id=device,
        device_id_type=pl.DeviceIdType.MESH,
    )


def kernel(
    nz, x_hbm, q_hbm, kv_hbm_in, o_hbm, cos_hbm, sin_hbm, dest_ref, length_ref, out_hbm, kv_hbm,
    wbuf, wobuf, xbuf, att, acc, oacc, obuf, meta, dests, srcv, srcs, kvall, swap, spread, perm, heads,
    meta_s, meta_r, w0_s, w0_r, ring_s, ring_r, sib_s, sib_r, y_s, y_r, own_s, own_r,
    o_s, o_r, osib_s, osib_r, oown_s, oown_r, x_l, x_s, xf_s, x_r, a_s, af_s, a_r, swap_s, swap_r,
    dest_s, dest_r, c1_s, c1_r, src_l, c2_s, c2_r, c3_s, c3_r, c3_l, out_s, out_r, out_l, ready, kvbuf, relay, relay_s, relay_r,
    oy_s, oy_r, oysib_s, oysib_r, q_ref, kv_pair, kv_ref, o_t, cos_ref, sin_ref, load,
):
    part, dp, c = lax.axis_index("parts"), lax.axis_index("dp"), lax.axis_index("tensor")
    x, z = lax.div(dp, nz), lax.rem(dp, nz)
    half = nz // 2
    yb = lax.rem(part, 2)
    mate = part + 1 - 2 * yb
    rows = q_ref.shape[0]
    total = xbuf.shape[1]
    piece = total // nz
    last = 2 * (half - 1)

    def at_x(offset, core):
        return (part, lax.rem(x + offset + NX, NX) * nz + z, core)

    def at_z(where, core):
        return (part, x * nz + where, core)

    sibling = (part, dp, 1 - c)
    partner = (mate, dp, c)
    up, down = lax.rem(z + 1, nz), lax.rem(z + nz - 1, nz)

    loads = [
        pltpu.make_async_copy(src, dst, load.at[i])
        for i, (src, dst) in enumerate(
            ((kv_hbm_in, kv_pair), (q_hbm, q_ref), (o_hbm, o_t), (cos_hbm, cos_ref), (sin_hbm, sin_ref))
        )
    ]
    for copy in loads:
        copy.start()

    barrier = pltpu.get_barrier_semaphore()

    def greet(semaphore, device):
        pl.semaphore_signal(semaphore, inc=1, device_id=device, device_id_type=pl.DeviceIdType.MESH)

    greeted = [at_x(o, k) for o in range(1, NX) for k in (0, 1)] + [sibling, partner]
    for device in greeted:
        greet(barrier, device)
    pl.when(z != 0)(lambda: greet(barrier, at_z(up, c)))
    pl.when(z == 1)(lambda: greet(barrier, at_z(down, c)))
    loads[0].wait()
    pair = kv_pair[...].astype(jnp.float32)
    for i in (0, 1):
        kv_ref[:, 2 * HD * i : 2 * HD * (i + 1)] = pair[:, i, :].astype(jnp.bfloat16)
    pl.semaphore_wait(
        barrier, len(greeted) + jnp.where(z == 1, 0, 1) + jnp.where(z == 0, 1, 0)
    )
    pl.when(z != 1)(lambda: greet(ready.at[0], at_z(down, c)))
    loads[1].wait()
    pl.when(z == 0)(lambda: greet(ready.at[1], at_z(up, c)))

    columns = wbuf.shape[2]
    q_cols = columns - 2 * HD

    def w_block(xs, zs):
        return wbuf.at[xs, pl.ds(pl.multiple_of(zs * rows, rows), rows), :]

    def w0_parts(b):
        return (
            (q_ref, b * q_cols, 0, q_cols),
            (kv_ref, b * HD, q_cols, HD),
            (kv_ref, (2 + b) * HD, q_cols + HD, HD),
        )

    def w0(b):
        block = w_block(x, z)
        return [
            remote(
                src.at[:, pl.ds(start, size)], block.at[:, pl.ds(to, size)], w0_s.at[b, i],
                w0_r.at[lax.rem(x, 2)], (part, (2 * c + b) * nz + z, lax.div(x, 2)),
            )
            for i, (src, start, to, size) in enumerate(w0_parts(b))
        ]

    for b in (0, 1):
        @pl.when(2 * c + b != x)
        def _(b=b):
            for copy in w0(b):
                copy.start()

    for b in (0, 1):
        @pl.when(2 * c + b == x)
        def _(b=b):
            block = w_block(x, z)
            for src, start, to, size in w0_parts(b):
                block[:, to : to + size] = src[:, start : start + size]

    meta[x] = jnp.concatenate(
        [jnp.full((1, HD), dest_ref[0], jnp.int32), jnp.full((1, HD), length_ref[0], jnp.int32)]
    )

    def meta_copy(o):
        return remote(meta.at[x], meta.at[x], meta_s.at[o], meta_r.at[o], at_x(o, c))

    for o in range(1, NX):
        meta_copy(o).start()

    quarter = total // 4

    def away(s):
        return lax.rem(x - 2 * c - s + 2 * NX, NX)

    is_source = lax.div(x, 2) == c
    mine = lax.rem(x, 2)

    def x_rows(q):
        return pl.ds(q * quarter, quarter)

    def x_send(direction, q):
        return remote(
            x_hbm.at[x_rows(q)], xbuf.at[mine, x_rows(q)], x_s.at[direction, q], x_r.at[mine, q],
            at_x(1 if direction == 0 else -1, c),
        )

    def x_local():
        return pltpu.make_async_copy(x_hbm, xbuf.at[mine], x_l)

    def x_forward(s, q, direction):
        return remote(
            xbuf.at[s, x_rows(q)], xbuf.at[s, x_rows(q)], xf_s.at[s, q % 2], x_r.at[s, q],
            at_x(1 if direction == 0 else -1, c),
        )

    @pl.when(is_source)
    def _():
        for i in range(4):
            x_send(0, i).start()
            x_send(1, (i + 2) % 4).start()
        x_local().start()

    def x_arrival(s, q):
        rows_of = xbuf.at[s, x_rows(q)]
        return remote(rows_of, rows_of, xf_s.at[s, q % 2], x_r.at[s, q], sibling)

    def pass_on(i):
        for s in (0, 1):
            @pl.when(away(s) == 1)
            def _(s=s):
                x_forward(s, i, 0).wait_recv()
                x_forward(s, i, 0).start()

            @pl.when(away(s) == 3)
            def _(s=s):
                x_forward(s, 2 + i, 1).wait_recv()
                x_forward(s, 2 + i, 1).start()

    def w_part(zs, core, which):
        cols = pl.ds(q_cols, 2 * HD)
        if which:
            at = yb if which == 1 else 1 - yb
            cols = pl.ds(pl.multiple_of(at * (q_cols // 2), q_cols // 2), q_cols // 2)
        return wbuf.at[pl.ds(2 * core, 2), pl.ds(pl.multiple_of(zs * rows, rows), rows), cols]

    def hop(direction, zs, idx, which):
        blk = w_part(zs, c, which)
        return remote(
            blk, blk, ring_s, ring_r.at[idx, which],
            at_z(up if direction == 0 else down, c),
        )

    def to_sibling(zs, idx, which):
        blk = w_part(zs, c, which)
        return remote(blk, blk, sib_s, sib_r.at[which], sibling)

    def to_partner(zs, idx):
        blk = w_part(zs, c, 1)
        return remote(blk, blk, y_s, y_r.at[idx], partner)

    def from_partner(zs, idx):
        blk = w_part(zs, c, 2)
        return remote(blk, blk, y_s, y_r.at[idx], partner)

    def own_to_sibling():
        blk = wbuf.at[pl.ds(2 * c, 2), pl.ds(pl.multiple_of(z * rows, rows), rows), :]
        return remote(blk, blk, own_s, own_r, sibling)

    def o_block(zs, core):
        return wobuf.at[core, pl.ds(pl.multiple_of(zs * QC, QC), QC), :]

    def o_part(zs, which):
        start = pl.multiple_of(zs * QC + which * (QC // 2), QC // 2)
        return wobuf.at[c, pl.ds(start, QC // 2), :]

    def o_hop(direction, zs, idx, src=None):
        blk = o_part(zs, yb)
        return remote(
            blk if src is None else src, blk, o_s, o_r.at[idx],
            at_z(up if direction == 0 else down, c),
        )

    def o_sibling(zs, idx):
        blk = o_part(zs, yb)
        return remote(blk, blk, osib_s, osib_r, sibling)

    def o_partner(zs, idx):
        blk = o_part(zs, yb)
        return remote(blk, blk, oy_s, oy_r, partner)

    def o_y_sibling(zs, idx):
        blk = o_part(zs, 1 - yb)
        return remote(blk, blk, oysib_s, oysib_r, sibling)

    def o_own_sibling():
        return remote(o_t, o_block(z, c), oown_s, oown_r, sibling)

    for i in (0, 1):
        @pl.when(2 * c + i != x)
        def _(i=i):
            blk = w_block(2 * c + i, z)
            remote(blk, blk, w0_s.at[0, 0], w0_r.at[i], sibling).wait_recv()

    first = (0, half - 1)
    own_to_sibling().start()
    pl.when(z != 0)(lambda: pl.semaphore_wait(ready.at[0], 1))
    for h in (0, 1):
        hop(0, z, first[0], h).start()
    pl.when(z == 1)(lambda: pl.semaphore_wait(ready.at[1], 1))
    for h in (0, 1):
        hop(1, z, first[1], h).start()
    loads[2].wait()
    o_block(z, c)[...] = o_t[...]

    def block_of(direction, k):
        return lax.rem(z + (nz - k if direction == 0 else k), nz)

    def slot_of(direction, k):
        return direction * (half - 1) + k - 1

    def partner_on(direction, k, idx):
        zs = block_of(direction, k)
        from_partner(zs, idx).wait_recv()
        to_sibling(zs, idx, 2).start()

    def w_half(direction, k, h):
        idx = slot_of(direction, k)
        zs = block_of(direction, k)
        hop(direction, zs, idx, h).wait_recv()

        @pl.when((k < half - 1) | (c == direction))
        def _():
            hop(direction, zs, jnp.where(k == half - 1, last, idx + 1), h).start()

    def w_rest(direction, k):
        idx = slot_of(direction, k)
        zs = block_of(direction, k)
        to_sibling(zs, idx, 0).start()
        to_sibling(zs, idx, 1).start()
        to_partner(zs, idx).start()

    def o_step(k):
        for direction in (0, 1):
            idx = slot_of(direction, k)
            zs = block_of(direction, k)
            o_hop(direction, zs, idx).wait_recv()

            @pl.when((k < half - 1) | (c == direction))
            def _(direction=direction, idx=idx, zs=zs):
                o_hop(direction, zs, jnp.where(k == half - 1, last, idx + 1)).start()

            o_sibling(zs, idx).start()
            if direction == 0:
                o_partner(zs, idx).start()

    def ring_step(k, carry):
        for h in (0, 1):
            for direction in (0, 1):
                w_half(direction, k, h)
        for direction in (0, 1):
            w_rest(direction, k)
        @pl.when(k > LAG)
        def _():
            o_step(k - LAG)

        @pl.when(k > Y_LAG)
        def _():
            for direction in (0, 1):
                partner_on(direction, k - Y_LAG, slot_of(direction, k - Y_LAG))

        return carry

    for direction in (0, 1):
        o_hop(direction, z, first[direction], o_t.at[pl.ds(pl.multiple_of(yb * (QC // 2), QC // 2), QC // 2)]).start()
    o_own_sibling().start()
    lax.fori_loop(1, 3, ring_step, 0)
    pass_on(0)
    lax.fori_loop(3, 5, ring_step, 0)
    pass_on(1)
    lax.fori_loop(5, half, ring_step, 0)
    far = block_of(0, half)
    for which in (0, 1):
        hop(0, far, last, which).wait_recv()
        to_sibling(far, last, which).start()
    to_partner(far, last).start()

    def w_all(start, size, semaphores):
        blk = wbuf.at[pl.ds(0, 2), pl.ds(0, (nz - 1) * rows), pl.ds(start, size)]
        return remote(blk, blk, *semaphores, sibling)

    w_all(q_cols, 2 * HD, (sib_s, sib_r.at[0])).wait_recv()
    own_to_sibling().wait_recv()
    for o in range(1, NX):
        meta_copy(o).wait_recv()

    lane = lax.broadcasted_iota(jnp.int32, (1, HD), 1)
    row = jnp.zeros((1, HD), jnp.int32)
    for j in range(NX):
        row = jnp.where(lane == j, meta[j, pl.ds(0, 1), :], row)
    dests[z] = row

    for copy in loads[3:]:
        copy.wait()
    cosine, sine = cos_ref[...], sin_ref[...]

    def rotated(u):
        return u * cosine + pltpu.roll(u, HD // 2, 1) * sine

    groups = q_cols // HD
    key_at = lax.broadcasted_iota(jnp.int32, (total, total), 1)
    query_at = lax.broadcasted_iota(jnp.int32, (total, total), 0)
    position = lax.broadcasted_iota(jnp.int32, (total, HD), 0)

    def a_send(s, direction):
        return remote(
            att.at[s, x], att.at[s, x], a_s.at[s, direction], a_r.at[s, direction],
            at_x(1 if direction == 0 else -1, c),
        )

    def a_forward(s, direction):
        source = lax.rem(x + (NX - 1 if direction == 0 else 1), NX)
        blk = att.at[s, source, pl.ds(direction * (total // 2), total // 2)]
        return remote(
            blk, blk, af_s.at[s, direction], a_r.at[s, 2 + direction],
            at_x(1 if direction == 0 else -1, c),
        )

    def pass_attended(s):
        for direction in (0, 1):
            a_send(s, direction).wait_recv()
        for direction in (0, 1):
            a_forward(s, direction).start()

    def x_wait(s):
        @pl.when(away(s) == 0)
        def _():
            x_local().wait()

        @pl.when((away(s) == 1) | (away(s) == 2))
        def _():
            for q in (2, 3):
                x_arrival(s, q).wait_recv()

        @pl.when((away(s) == 3) | (away(s) == 2))
        def _():
            for q in (0, 1):
                x_arrival(s, q).wait_recv()

    def project(start, size):
        cols = pl.ds(start, size)
        per = nz * rows // KC

        def part_of(i):
            deep = pl.ds(pl.multiple_of(i * KC, KC), KC)
            inside = pl.ds(pl.multiple_of(lax.rem(i, per) * KC, KC), KC)
            both = xbuf[:, :, deep].reshape(2 * total, KC)
            return jnp.dot(
                both, wbuf[lax.div(i, per), inside, cols], preferred_element_type=jnp.float32
            ).reshape(2, total, size)

        acc[:, :, cols] = part_of(0)

        def add(i, carry):
            acc[:, :, cols] += part_of(i)
            return carry

        lax.fori_loop(1, xbuf.shape[2] // KC, add, 0)

    def cache_rows(s):
        length = meta[2 * c + s, pl.ds(1, 1), :]
        keys = rotated(acc[s, :, q_cols : q_cols + HD])
        values = acc[s, :, q_cols + HD :]
        live = position < length
        kept_keys = jnp.where(live, keys, 0.0).astype(jnp.bfloat16)
        kept_values = jnp.where(live, values, 0.0).astype(jnp.bfloat16)

        @pl.when(c == 0)
        def _():
            kvall[s] = kept_keys
            swap[s] = kept_values

        @pl.when(c == 1)
        def _():
            kvall[2 + s] = kept_values
            swap[s] = kept_keys

        kvbuf[s, 0] = keys.astype(jnp.bfloat16)
        kvbuf[s, 1] = values.astype(jnp.bfloat16)

    def attend(s):
        keys, values = kvbuf[s, 0], kvbuf[s, 1]
        length = meta[2 * c + s, pl.ds(1, 1), :]
        wide = jnp.concatenate([length] * (total // HD), axis=1)
        allowed = (query_at >= key_at) & (key_at < wide)
        for g in range(groups):
            query = rotated(acc[s, :, g * HD : (g + 1) * HD]).astype(jnp.bfloat16)
            scores = lax.dot_general(
                query, keys, (((1,), (1,)), ((), ())), preferred_element_type=jnp.float32
            ) * (1.0 / math.sqrt(HD))
            scores = jnp.where(allowed, scores, -jnp.inf)
            expo = jnp.exp(scores - jnp.max(scores, axis=1, keepdims=True))
            weights = (expo / jnp.sum(expo, axis=1, keepdims=True)).astype(jnp.bfloat16)
            att[s, x, :, g * HD : (g + 1) * HD] = jnp.dot(
                weights, values, preferred_element_type=jnp.float32
            ).astype(jnp.bfloat16)
        for direction in (0, 1):
            a_send(s, direction).start()

    def swapped(s):
        return remote(swap.at[s], kvall.at[2 * c + s], swap_s.at[s], swap_r.at[s], sibling)

    def d_copy(o):
        return remote(dests.at[z], dests.at[z], dest_s, dest_r, at_z(lax.rem(z + o, nz), c))

    def c1_copy(o):
        to = lax.rem(z + o, nz)
        return remote(
            kvall.at[:, pl.ds(pl.multiple_of(to * piece, piece), piece), :],
            spread.at[pl.ds(z * NX, NX)],
            c1_s, c1_r, at_z(to, c),
        )

    def send_dest(o, carry):
        d_copy(o).start()
        return carry

    def send_c1(o, carry):
        c1_copy(o).start()
        return carry

    for s in (0, 1):
        x_wait(s)
    project(q_cols, 2 * HD)
    for s in (0, 1):
        cache_rows(s)
        swapped(s).start()
    for k in range(half - LAG, half):
        o_step(k)
    def o_over(k, carry):
        o_partner(block_of(1, k), slot_of(1, k)).start()
        return carry

    lax.fori_loop(1, half, o_over, 0)

    for k in range(half - Y_LAG, half):
        for direction in (0, 1):
            partner_on(direction, k, slot_of(direction, k))
    partner_on(0, half, last)
    for s in (0, 1):
        swapped(s).wait_recv()
    lax.fori_loop(1, nz, send_c1, 0)
    spread[pl.ds(z * NX, NX)] = kvall[:, pl.ds(pl.multiple_of(z * piece, piece), piece), :]
    for which in (1, 2):
        w_all(0, q_cols // 2, (sib_s, sib_r.at[which])).wait_recv()
    project(0, q_cols)
    lax.fori_loop(1, nz, send_dest, 0)
    o_hop(0, far, last).wait_recv()
    o_sibling(far, last).start()
    o_partner(far, last).start()
    attend(0)
    attend(1)
    pass_attended(0)
    def d_all():
        blk = dests.at[pl.ds(0, nz - 1)]
        return remote(blk, blk, dest_s, dest_r, sibling)

    def c1_all():
        blk = spread.at[pl.ds(0, NX * (nz - 1))]
        return remote(blk, blk, c1_s, c1_r, sibling)

    d_all().wait_recv()
    c1_all().wait_recv()
    all_dests = dests[...].reshape(nz, HD)
    lanes = lax.broadcasted_iota(jnp.int32, (nz, HD), 1)
    prompt = lax.broadcasted_iota(jnp.int32, (nz, HD), 0) * NX
    source = jnp.zeros((nz, HD), jnp.int32)
    for j in range(NX):
        slot = jnp.sum(jnp.where(lanes == j, all_dests, 0), axis=1, keepdims=True)
        source += jnp.where(slot == lanes, prompt + j, 0)
    srcv[...] = jnp.minimum(jnp.sum(source, axis=0, keepdims=True), NX * nz - 1)
    to_scalars = pltpu.make_async_copy(srcv, srcs, src_l)
    to_scalars.start()
    to_scalars.wait()

    def reorder(d, carry):
        for j in range(NX):
            perm[j, d] = spread[srcs[0, j * nz + d]]
        return carry

    lax.fori_loop(0, nz, reorder, 0, unroll=4)

    def c2_copy(o):
        to = lax.rem(z + o, nz)
        return remote(perm.at[:, to], heads.at[:, z], c2_s, c2_r, at_z(to, c))

    def send_c2(o, carry):
        c2_copy(o).start()
        return carry

    lax.fori_loop(1, nz, send_c2, 0)
    heads[:, z] = perm[:, z]
    def o_all(semaphores):
        blk = wobuf.at[c, pl.ds(0, (nz - 1) * (QC // 2)), :]
        return remote(blk, blk, *semaphores, sibling)

    o_all((oy_s, oy_r)).wait_recv()

    def o_crossed(idx, carry):
        zs = jnp.where(
            idx == last, far,
            jnp.where(idx < half - 1, block_of(0, idx + 1), block_of(1, idx + 2 - half)),
        )
        o_y_sibling(zs, idx).start()
        return carry

    lax.fori_loop(0, last + 1, o_crossed, 0)

    pass_attended(1)
    o_all((osib_s, osib_r)).wait_recv()
    o_all((oysib_s, oysib_r)).wait_recv()
    o_own_sibling().wait_recv()

    def head_rows(s, xs):
        core = lax.div(xs, 2)
        cols = pl.ds(pl.multiple_of(lax.rem(xs, 2) * q_cols, q_cols), q_cols)
        return lax.dot_general(
            att[s, xs], wobuf[core, :, cols], (((1,), (1,)), ((), ())),
            preferred_element_type=jnp.float32,
        )

    for s in (0, 1):
        oacc[s] = head_rows(s, x)
        for direction in (0, 1):
            oacc[s] += head_rows(s, lax.rem(x + (NX - 1 if direction == 0 else 1), NX))

    width = oacc.shape[2]

    def out_cols(xs):
        return pl.ds(pl.multiple_of(lax.rem(xs, 2) * width, width), width)

    def out_copy(s):
        return remote(
            obuf.at[s], out_hbm.at[:, out_cols(x)], out_s.at[s, 0], out_r.at[lax.rem(x, 2)],
            (part, (2 * c + s) * nz + z, lax.div(x, 2)),
        )

    def out_here(s):
        return pltpu.make_async_copy(obuf.at[s], out_hbm.at[:, out_cols(x)], out_l)

    def out_rows(direction):
        return pl.ds(direction * (total // 2), total // 2)

    def out_first(s, direction):
        return remote(
            obuf.at[s, out_rows(direction)], relay.at[direction], out_s.at[s, direction],
            relay_r.at[direction], at_x(1 if direction == 0 else -1, c),
        )

    def out_second(direction):
        source = lax.rem(x + (NX - 1 if direction == 0 else 1), NX)
        return remote(
            relay.at[direction], out_hbm.at[out_rows(direction), out_cols(source)],
            relay_s.at[direction], out_r.at[lax.rem(source, 2)],
            at_x(1 if direction == 0 else -1, lax.div(source, 2)),
        )

    def relays(direction):
        to = lax.rem(x + (1 if direction == 0 else NX - 1), NX)
        return lax.div(to, 2) == c

    for s in (0, 1):
        for direction in (0, 1):
            a_forward(s, direction).wait_recv()
        obuf[s] = (oacc[s] + head_rows(s, lax.rem(x + 2, NX))).astype(jnp.bfloat16)

        @pl.when(away(s) == 2)
        def _(s=s):
            for direction in (0, 1):
                out_first(s, direction).start()

        pl.when((away(s) == 1) | (away(s) == 3))(lambda s=s: out_copy(s).start())
        pl.when(away(s) == 0)(lambda s=s: out_here(s).start())

    for direction in (0, 1):
        @pl.when(relays(direction))
        def _(direction=direction):
            out_first(0, direction).wait_recv()
            out_second(direction).start()

    def c2_all():
        blk = heads.at[:, pl.ds(0, nz - 1)]
        return remote(blk, blk, c2_s, c2_r, sibling)

    c2_all().wait_recv()

    def c3_copy(o, t):
        return remote(
            heads.at[lax.rem(x + o, NX), pl.ds(t * half, half)], kv_hbm.at[c, x, :, :, :],
            c3_s, c3_r, at_x(o, t),
        )

    def c3_here():
        return pltpu.make_async_copy(heads.at[x, pl.ds(c * half, half)], kv_hbm.at[c, x, :, :, :], c3_l)

    for o in range(1, NX):
        for t in (0, 1):
            c3_copy(o, t).start()
    c3_copy(0, 1 - c).start()
    c3_here().start()

    def c3_all():
        blk = heads.at[:, pl.ds(0, (2 * NX - 1) * half // NX)]
        return remote(blk, blk, c3_s, c3_r, sibling)

    c3_all().wait_recv()
    c3_here().wait()
    c3_all().wait_send()
    for i in (0, 1):
        @pl.when(2 * c + i != x)
        def _(i=i):
            cols = pl.ds(i * width, width)
            remote(obuf.at[0], out_hbm.at[:, cols], out_s.at[0, 0], out_r.at[i], sibling).wait_recv()

    for s in (0, 1):
        @pl.when(away(s) == 2)
        def _(s=s):
            for direction in (0, 1):
                out_first(s, direction).wait_send()

        pl.when((away(s) == 1) | (away(s) == 3))(lambda s=s: out_copy(s).wait_send())
        pl.when(away(s) == 0)(lambda s=s: out_here(s).wait())
        pl.when(relays(s))(lambda s=s: out_second(s).wait_send())
        for direction in (0, 1):
            a_send(s, direction).wait_send()
        for direction in (0, 1):
            a_forward(s, direction).wait_send()
    for b in (0, 1):
        @pl.when(2 * c + b != x)
        def _(b=b):
            for copy in w0(b):
                copy.wait_send()

    for o in range(1, NX):
        meta_copy(o).wait_send()

    @pl.when(is_source)
    def _():
        for i in range(4):
            for direction in (0, 1):
                x_send(direction, i).wait_send()

    for s in (0, 1):
        for i in (0, 1):
            pl.when(away(s) == 1)(lambda s=s, i=i: x_forward(s, i, 0).wait_send())
            pl.when(away(s) == 3)(lambda s=s, i=i: x_forward(s, 2 + i, 1).wait_send())
        swapped(s).wait_send()
    own_to_sibling().wait_send()
    o_own_sibling().wait_send()

    for sent in (d_all(), c1_all(), c2_all()):
        sent.wait_send()
    w_all(0, q_cols, (ring_s, ring_r.at[0, 0])).wait_send()
    w_all(0, columns, (sib_s, sib_r.at[0])).wait_send()
    w_all(0, q_cols // 2, (y_s, y_r.at[0])).wait_send()
    for pair in ((o_s, o_r.at[0]), (osib_s, osib_r), (oy_s, oy_r), (oysib_s, oysib_r)):
        o_all(pair).wait_send()


def on_device(normed, q_weight, kv_weight, o_weight, lengths, destinations):
    tokens = normed[0]
    total, width = tokens.shape
    nz = lax.axis_size("dp") // NX
    rows = q_weight.shape[0]
    q_cols = q_weight.shape[1] // 2
    o_t = o_weight.T
    cosine, sine = tables(total)
    columns = q_cols + 2 * HD
    o_cols = rows * nz
    piece = total // nz
    hops = nz - 1
    bf16, f32 = jnp.bfloat16, jnp.float32
    dma = pltpu.SemaphoreType.DMA
    scratch = [
        pltpu.VMEM((NX, width // NX, columns), bf16),
        pltpu.VMEM((2, o_cols, o_weight.shape[0]), bf16),
        pltpu.VMEM((2, total, width), bf16),
        pltpu.VMEM((2, NX, total, q_cols), bf16),
        pltpu.VMEM((2, total, columns), f32),
        pltpu.VMEM((2, total, o_cols), f32),
        pltpu.VMEM((2, total, o_cols), bf16),
        pltpu.VMEM((NX, 2, HD), jnp.int32),
        pltpu.VMEM((nz, 1, HD), jnp.int32),
        pltpu.VMEM((1, HD), jnp.int32),
        pltpu.SMEM((1, HD), jnp.int32),
        pltpu.VMEM((NX, total, HD), bf16),
        pltpu.VMEM((2, total, HD), bf16),
        pltpu.VMEM((NX * nz, piece, HD), bf16),
        pltpu.VMEM((NX, nz, piece, HD), bf16),
        pltpu.VMEM((NX, nz, piece, HD), bf16),
    ]
    shapes = [
        (NX,), (NX,), (2, 3), (2,), None, (hops, 2), None, (3,), None, (hops,), None, None,
        None, (hops,), None, None, None, None, None, (2, 4), (2, 2), (2, 4), (2, 2), (2, 2), (2, 4), (2,), (2,),
        None, None, None, None, None, None, None, None, None, None, (2, 2), (2,), None,
    ]
    scratch += [dma if shape is None else dma(shape) for shape in shapes]
    scratch.append(pltpu.SemaphoreType.REGULAR((2,)))
    scratch += [pltpu.VMEM((2, 2, total, HD), bf16), pltpu.VMEM((2, total // 2, o_cols), bf16), dma((2,)), dma((2,))]
    scratch += [dma] * 4
    scratch += [pltpu.VMEM(a.shape, a.dtype) for a in (q_weight, kv_weight, kv_weight.reshape(rows, -1), o_t, cosine, sine)]
    scratch.append(dma((5,)))
    smem = pl.BlockSpec(memory_space=pltpu.SMEM)
    vmem = pl.BlockSpec(memory_space=pltpu.VMEM)
    any_space = pl.BlockSpec(memory_space=pl.ANY)
    projected, cache = pl.pallas_call(
        functools.partial(kernel, nz),
        out_shape=(
            pltpu.VMEM((total, 2 * o_cols), bf16),
            pltpu.VMEM((2, NX, nz // 2, piece, HD), bf16),
        ),
        in_specs=[any_space] * 6 + [smem, smem],
        out_specs=(vmem, vmem),
        scratch_shapes=scratch,
        compiler_params=pltpu.CompilerParams(
            collective_id=0, has_side_effects=True, vmem_limit_bytes=60 * 1024 * 1024
        ),
    )(tokens, q_weight, kv_weight, o_t, cosine, sine, destinations, lengths)
    return (projected[None], cache.reshape(1, 2, NX, total // 2, HD))


def solution(mesh):
    placed = (
        P(("parts", "dp"), None, None),
        P("dp", "tensor"),
        P("dp", None, "tensor"),
        P("tensor", "dp"),
        P(("parts", "dp")),
        P(("parts", "dp")),
    )
    return jax.shard_map(
        on_device,
        mesh=mesh,
        in_specs=placed,
        out_specs=(
            P(("parts", "dp"), None, "tensor"),
            P(("parts", "dp"), None, None, "tensor", None),
        ),
        check_vma=False,
    )
```
